16 devices in a mesh: dp: 2 (over y, z), tp: 8 (over x, core).
Axes of the slice: x: 4, y: 2, z: 1, core: 2. Of those that a mesh axis runs over, the one named last changes fastest.
The devices are a block of a 4x4x8 slice.
Arguments:
- y_one: float32 [16, 32, 2048], P('dp'), parts along dimension 0
- y_two: float32 [16, 32, 2048], P('dp'), parts along dimension 0
- dy_one: float32 [16, 32, 2048], P('dp'), parts along dimension 0
- dy_two: float32 [16, 32, 2048], P('dp'), parts along dimension 0
- seq_lens: int32 [16], P('dp'), parts along dimension 0
- w_query: bfloat16 [4, 2048, 32, 64], P(None, None, 'tp')
- w_key: bfloat16 [4, 2048, 8, 64], P(None, None, 'tp')
- w_value: bfloat16 [4, 2048, 8, 64], P(None, None, 'tp')
- w_out: bfloat16 [4, 32, 64, 2048], P(None, 'tp')
- w_up: bfloat16 [4, 2048, 5632], P(None, None, 'tp')
- w_down: bfloat16 [4, 5632, 2048], P(None, 'tp')
Outputs:
- output 1: float32 [16, 32, 2048], P('dp'), parts along dimension 0
- output 2: float32 [16, 32, 2048], P('dp'), parts along dimension 0
- output 3: float32 [16, 32, 2048], P('dp'), parts along dimension 0
- output 4: float32 [16, 32, 2048], P('dp'), parts along dimension 0
- output 5: float32 [8, 2048, 32, 64], P('dp', None, 'tp'), parts along dimension 0
- output 6: float32 [8, 2048, 8, 64], P('dp', None, 'tp'), parts along dimension 0
- output 7: float32 [8, 2048, 8, 64], P('dp', None, 'tp'), parts along dimension 0
- output 8: float32 [8, 32, 64, 2048], P('dp', 'tp'), parts along dimension 0
- output 9: float32 [8, 2048, 5632], P('dp', None, 'tp'), parts along dimension 0
- output 10: float32 [8, 5632, 2048], P('dp', 'tp'), parts along dimension 0
There are 2 independent parts. The reference program is written for one: setup_inputs(seed, part) draws one part's arguments, and reference() takes and returns one part's arrays. A program takes and returns all parts, laid end to end along the dimension named above; an argument that names none is the same for every part.
All inputs are finite; a program needn't handle non-finite values.
Results may differ from the reference program's by a relative error of at most 0.02.
Values are sent between devices in bfloat16 or wider.
A program may use at most 768 MiB of HBM per device.

```python
import functools
import jax
import jax.numpy as jnp
from jax import lax

D = 2048
HEADS = 32
KV_HEADS = 4
HEAD = 64
FF = 5632
LAYERS = 4
SEQS = 1
SEQ = 32
TP = 8
KV_SLOTS = max(KV_HEADS, TP)
REPEAT = KV_SLOTS // KV_HEADS
GROUP = HEADS // KV_SLOTS
BATCH = SEQS * TP
TOKENS = BATCH * SEQ
EPS = 1e-5
SCORE_SCALE = HEAD ** -0.5
OUT_GAIN = 0.5 * (SEQ / 64) ** 0.25


def normal_weights(rng_key, arr_shape, scale_std):
    return (jax.random.normal(rng_key, arr_shape, jnp.float32) * scale_std).astype(jnp.bfloat16)


def draw_lengths(rng_key):
    len_key, top_key, low_key = jax.random.split(rng_key, 3)
    seq_lens = jax.random.randint(len_key, (BATCH,), SEQ // 4, SEQ + 1)
    top_idx = jax.random.randint(top_key, (), 0, BATCH)
    low_idx = (top_idx + jax.random.randint(low_key, (), 1, BATCH)) % BATCH
    positions = jnp.arange(BATCH)
    seq_lens = jnp.where(positions == top_idx, SEQ, seq_lens)
    seq_lens = jnp.where(positions == low_idx, SEQ // 4, seq_lens)
    return seq_lens.astype(jnp.int32)


def setup_inputs(seed: int = 0, part: int = 0) -> dict:
    weight_keys = jax.random.split(jax.random.key(seed), 6)
    part_keys = jax.random.split(jax.random.fold_in(jax.random.key(seed + 1), part), 5)
    act_shape = (BATCH, SEQ, D)
    key_heads = normal_weights(weight_keys[1], (LAYERS, D, KV_HEADS, HEAD), D ** -0.5)
    value_heads = normal_weights(weight_keys[2], (LAYERS, D, KV_HEADS, HEAD), D ** -0.5)
    return {
        'y_one': jax.random.normal(part_keys[0], act_shape, jnp.float32),
        'y_two': jax.random.normal(part_keys[1], act_shape, jnp.float32),
        'dy_one': jax.random.normal(part_keys[2], act_shape, jnp.float32),
        'dy_two': jax.random.normal(part_keys[3], act_shape, jnp.float32),
        'seq_lens': draw_lengths(part_keys[4]),
        'w_query': normal_weights(weight_keys[0], (LAYERS, D, HEADS, HEAD), 2.0 * D ** -0.5),
        'w_key': jnp.repeat(key_heads, REPEAT, axis=2),
        'w_value': jnp.repeat(value_heads, REPEAT, axis=2),
        'w_out': normal_weights(weight_keys[3], (LAYERS, HEADS, HEAD, D), OUT_GAIN * (HEADS * HEAD) ** -0.5),
        'w_up': normal_weights(weight_keys[4], (LAYERS, D, FF), D ** -0.5),
        'w_down': normal_weights(weight_keys[5], (LAYERS, FF, D), 0.6 * FF ** -0.5),
    }


def rms_norm(x_val):
    inv_rms = lax.rsqrt(jnp.mean(x_val * x_val, axis=-1, keepdims=True) + EPS)
    return x_val * inv_rms, inv_rms


def rms_back(normed, inv_rms, grad_norm):
    return inv_rms * (grad_norm - normed * jnp.mean(grad_norm * normed, axis=-1, keepdims=True))


def attend_seq(operands):
    q_seq, k_seq, v_seq, dout_seq, seq_len = operands
    q_grp = q_seq.reshape(SEQ, KV_SLOTS, GROUP, HEAD).astype(jnp.float32)
    k_full = k_seq.astype(jnp.float32)
    v_full = v_seq.astype(jnp.float32)
    dout_grp = dout_seq.reshape(SEQ, KV_SLOTS, GROUP, HEAD).astype(jnp.float32)
    row_pos = jnp.arange(SEQ)[:, None]
    col_pos = jnp.arange(SEQ)[None, :]
    visible = (col_pos <= row_pos) & (col_pos < seq_len)
    scores = jnp.einsum('igre,jge->grij', q_grp, k_full) * SCORE_SCALE
    scores = jnp.where(visible, scores, -1e30)
    attn_probs = jax.nn.softmax(scores, axis=-1)
    probs_b = attn_probs.astype(jnp.bfloat16).astype(jnp.float32)
    attn_out = jnp.einsum('grij,jge->igre', probs_b, v_full).astype(jnp.bfloat16)
    d_value = jnp.einsum('grij,igre->jge', probs_b, dout_grp).astype(jnp.bfloat16)
    d_probs = jnp.einsum('igre,jge->grij', dout_grp, v_full)
    d_scores = attn_probs * (d_probs - jnp.sum(d_probs * attn_probs, axis=-1, keepdims=True)) * SCORE_SCALE
    d_scores = d_scores.astype(jnp.bfloat16).astype(jnp.float32)
    d_query = jnp.einsum('grij,jge->igre', d_scores, k_full).astype(jnp.bfloat16)
    d_key = jnp.einsum('grij,igre->jge', d_scores, q_grp).astype(jnp.bfloat16)
    return attn_out.reshape(SEQ, HEADS, HEAD), d_query.reshape(SEQ, HEADS, HEAD), d_key, d_value


def layer_back(seq_lens, carry, layer_w):
    y_one, y_two, dy_one, dy_two = carry
    w_query, w_key, w_value, w_out, w_up, w_down = layer_w
    norm_g, inv_g = rms_norm(y_one.reshape(TOKENS, D))
    norm_g_b = norm_g.astype(jnp.bfloat16)
    pre_act = jnp.dot(norm_g_b, w_up, preferred_element_type=jnp.float32)
    act_val, gelu_back = jax.vjp(jax.nn.gelu, pre_act)
    act_b = act_val.astype(jnp.bfloat16)
    g_branch = jnp.dot(act_b, w_down, preferred_element_type=jnp.float32)
    x_two = y_two - g_branch.reshape(BATCH, SEQ, D)
    dy2_b = dy_two.reshape(TOKENS, D).astype(jnp.bfloat16)
    d_act = jnp.dot(dy2_b, w_down.T, preferred_element_type=jnp.float32)
    d_pre = gelu_back(d_act)[0].astype(jnp.bfloat16)
    dw_down = jnp.dot(act_b.T, dy2_b, preferred_element_type=jnp.float32)
    dw_up = jnp.dot(norm_g_b.T, d_pre, preferred_element_type=jnp.float32)
    grad_norm_g = jnp.dot(d_pre, w_up.T, preferred_element_type=jnp.float32)
    dy_one = dy_one + rms_back(norm_g, inv_g, grad_norm_g).reshape(BATCH, SEQ, D)

    norm_f, inv_f = rms_norm(x_two.reshape(TOKENS, D))
    norm_f_b = norm_f.astype(jnp.bfloat16)
    wq_flat = w_query.reshape(D, HEADS * HEAD)
    wk_flat = w_key.reshape(D, KV_SLOTS * HEAD)
    wv_flat = w_value.reshape(D, KV_SLOTS * HEAD)
    wo_flat = w_out.reshape(HEADS * HEAD, D)
    q_all = jnp.dot(norm_f_b, wq_flat, preferred_element_type=jnp.float32).astype(jnp.bfloat16).reshape(BATCH, SEQ, HEADS, HEAD)
    k_all = jnp.dot(norm_f_b, wk_flat, preferred_element_type=jnp.float32).astype(jnp.bfloat16).reshape(BATCH, SEQ, KV_SLOTS, HEAD)
    v_all = jnp.dot(norm_f_b, wv_flat, preferred_element_type=jnp.float32).astype(jnp.bfloat16).reshape(BATCH, SEQ, KV_SLOTS, HEAD)
    dy1_b = dy_one.reshape(TOKENS, D).astype(jnp.bfloat16)
    d_attn = jnp.dot(dy1_b, wo_flat.T, preferred_element_type=jnp.float32).astype(jnp.bfloat16).reshape(BATCH, SEQ, HEADS, HEAD)
    attn_out, d_query, d_key, d_value = lax.map(attend_seq, (q_all, k_all, v_all, d_attn, seq_lens))
    out_flat = attn_out.reshape(TOKENS, HEADS * HEAD)
    f_branch = jnp.dot(out_flat, wo_flat, preferred_element_type=jnp.float32)
    x_one = y_one - f_branch.reshape(BATCH, SEQ, D)
    dw_out = jnp.dot(out_flat.T, dy1_b, preferred_element_type=jnp.float32).reshape(HEADS, HEAD, D)
    dq_flat = d_query.reshape(TOKENS, HEADS * HEAD)
    dk_flat = d_key.reshape(TOKENS, KV_SLOTS * HEAD)
    dv_flat = d_value.reshape(TOKENS, KV_SLOTS * HEAD)
    dw_query = jnp.dot(norm_f_b.T, dq_flat, preferred_element_type=jnp.float32).reshape(D, HEADS, HEAD)
    dw_key = jnp.dot(norm_f_b.T, dk_flat, preferred_element_type=jnp.float32).reshape(D, KV_SLOTS, HEAD)
    dw_value = jnp.dot(norm_f_b.T, dv_flat, preferred_element_type=jnp.float32).reshape(D, KV_SLOTS, HEAD)
    grad_norm_f = (jnp.dot(dq_flat, wq_flat.T, preferred_element_type=jnp.float32)
                   + jnp.dot(dk_flat, wk_flat.T, preferred_element_type=jnp.float32)
                   + jnp.dot(dv_flat, wv_flat.T, preferred_element_type=jnp.float32))
    dx_two = dy_two + rms_back(norm_f, inv_f, grad_norm_f).reshape(BATCH, SEQ, D)
    return (x_one, x_two, dy_one, dx_two), (dw_query, dw_key, dw_value, dw_out, dw_up, dw_down)


def reference(y_one, y_two, dy_one, dy_two, seq_lens, w_query, w_key, w_value, w_out, w_up, w_down):
    end_state, layer_grads = lax.scan(functools.partial(layer_back, seq_lens), (y_one, y_two, dy_one, dy_two), (w_query, w_key, w_value, w_out, w_up, w_down), reverse=True)
    return (end_state[0], end_state[1], end_state[2], end_state[3], layer_grads[0], layer_grads[1], layer_grads[2], layer_grads[3], layer_grads[4], layer_grads[5])
```

```python
import functools

import jax
import jax.numpy as jnp
from jax import lax
from jax.experimental import pallas as pl
from jax.experimental.pallas import tpu as pltpu
from jax.sharding import PartitionSpec as P

F32 = jnp.float32
BF16 = jnp.bfloat16
EPS = 1e-5
MASK_VALUE = -1e30
GELU_C = 0.7978845608028654
GELU_A = 0.044715
MESH = pl.DeviceIdType.MESH
NT = (((1,), (1,)), ((), ()))
NN = (((1,), (0,)), ((), ()))
TN = (((0,), (0,)), ((), ()))


def mm(lhs, rhs, dims):
    return lax.dot_general(lhs, rhs, dims, preferred_element_type=F32)


def chain_kernel(cfg, lens, y1_h, y2_h, dy1_h, dy2_h, w1_h, w2_h, wq_h, wk_h, wv_h, wo_h,
                 fin_h, n1_o, n2_o, c_o, e_o, h_o, u_o, a_o, d_o,
                 n1, n2, cc, ee, w1, w2, wqkv, wo, h_s, u_s, gp, qkv, att, dqkv, probs, mask,
                 x1, x2, dy1, dy2, part, ra, rb, rc,
                 w_sem, in_sem, out_sem, fin_sem, rs_send, rs_recv, ag_send, ag_recv):
    n_layers, tp, seq, width, heads, hd = cfg
    chips = tp // 2
    tokens = tp * seq
    half = seq // 2
    scale = hd ** -0.5
    qw = heads * hd
    me = lax.axis_index('tp')
    chip = me // 2
    core = me - 2 * chip
    partner = me + 1 - 2 * core
    right = lax.rem(me + 2, tp)
    left = lax.rem(me + tp - 2, tp)
    opp = lax.rem(me + chips, tp)

    def rows(start, size=seq):
        return pl.ds(pl.multiple_of(start, half), size)

    def blk(ref, who):
        return ref.at[rows(who * seq)]

    def blk_a(ref, who):
        return ref.at[rows(who * seq, half)]

    def blk_b(ref, who):
        return ref.at[rows(who * seq + half, half)]

    def rcopy(src, dst, send, recv, dev):
        return pltpu.make_async_remote_copy(src_ref=src, dst_ref=dst, send_sem=send, recv_sem=recv,
                                            device_id={'tp': dev}, device_id_type=MESH)

    def w_copies(step):
        layer = n_layers - 1 - step
        slot = lax.rem(step, 2)
        kw = wk_h.shape[1]
        return (pltpu.make_async_copy(w1_h.at[layer], w1.at[slot], w_sem.at[slot, 0]),
                pltpu.make_async_copy(w2_h.at[layer], w2.at[slot], w_sem.at[slot, 1]),
                pltpu.make_async_copy(wq_h.at[layer], wqkv.at[slot, pl.ds(0, qw)], w_sem.at[slot, 2]),
                pltpu.make_async_copy(wk_h.at[layer], wqkv.at[slot, pl.ds(qw, kw)], w_sem.at[slot, 3]),
                pltpu.make_async_copy(wv_h.at[layer], wqkv.at[slot, pl.ds(qw + kw, kw)], w_sem.at[slot, 4]),
                pltpu.make_async_copy(wo_h.at[layer], wo.at[slot], w_sem.at[slot, 5]))

    owners = (opp, right, left, me)

    def rs_d2d(i, role):
        own = owners[role]
        theirs = own + 1 - 2 * core
        return rcopy(blk(part.at[i], theirs), ra.at[i, role], rs_send.at[i, role], rs_recv.at[i, role], partner)

    def rs_ring(i, kind):
        pt = part.at[i]
        lo, hi = pl.ds(0, half), pl.ds(half, half)
        src, dst, dev = ((blk_a(pt, opp), rb.at[i, 0], right), (blk_b(pt, opp), rb.at[i, 1], left),
                         (blk_b(pt, right), rc.at[i, 0, hi], right), (blk_a(pt, left), rc.at[i, 1, lo], left),
                         (blk_a(pt, right), rc.at[i, 0, lo], right), (blk_b(pt, left), rc.at[i, 1, hi], left))[kind]
        return rcopy(src, dst, rs_send.at[i, 4 + kind], rs_recv.at[i, 4 + kind], dev)

    def rs_add(i, who, extra, off=0, size=seq):
        where_rows = rows(who * seq + off, size)
        part[i, where_rows, :] = part[i, where_rows, :] + extra

    def rs_a(i):
        for role in range(4):
            rs_d2d(i, role).start()

    def rs_b(i):
        rs_d2d(i, 0).wait_recv()
        rs_add(i, opp, ra[i, 0])
        rs_ring(i, 0).start()
        rs_ring(i, 1).start()

    def rs_c(i):
        rs_d2d(i, 1).wait_recv()
        rs_add(i, right, ra[i, 1])
        rs_ring(i, 2).start()
        rs_d2d(i, 2).wait_recv()
        rs_add(i, left, ra[i, 2])
        rs_ring(i, 3).start()

    def rs_d(i):
        rs_ring(i, 0).wait_recv()
        rs_add(i, right, rb[i, 0], 0, half)
        rs_ring(i, 4).start()
        rs_ring(i, 1).wait_recv()
        rs_add(i, left, rb[i, 1], half, half)
        rs_ring(i, 5).start()

    def rs_e(i):
        rs_d2d(i, 3).wait_recv()
        for kind in range(2, 6):
            rs_ring(i, kind).wait_recv()
        for role in range(4):
            rs_d2d(i, role).wait_send()
        for kind in range(6):
            rs_ring(i, kind).wait_send()
        return (part[i, rows(me * seq), :] + ra[i, 3]) + (rc[i, 0] + rc[i, 1])

    bufs = (n2, cc, n1, ee)

    def ag_msg(i, kind, receive=False):
        buf = bufs[i]
        if receive:
            p_left = lax.rem(partner + tp - 2, tp)
            p_right = lax.rem(partner + 2, tp)
            p_opp = lax.rem(partner + chips, tp)
            ref = (lambda: blk(buf, left), lambda: blk(buf, right), lambda: blk(buf, partner), lambda: blk_a(buf, opp),
                   lambda: blk_b(buf, opp), lambda: blk(buf, p_left), lambda: blk(buf, p_right),
                   lambda: blk_a(buf, p_opp), lambda: blk_b(buf, p_opp))[kind]()
        else:
            ref = (lambda: blk(buf, me), lambda: blk(buf, me), lambda: blk(buf, me), lambda: blk_a(buf, left),
                   lambda: blk_b(buf, right), lambda: blk(buf, left), lambda: blk(buf, right),
                   lambda: blk_a(buf, opp), lambda: blk_b(buf, opp))[kind]()
        dev = (right, left, partner, right, left, partner, partner, partner, partner)[kind]
        return rcopy(ref, ref, ag_send.at[i, kind], ag_recv.at[i, kind], dev)

    def ag_f(i):
        for kind in range(3):
            ag_msg(i, kind).start()

    def ag_g(i):
        ag_msg(i, 0, True).wait_recv()
        ag_msg(i, 3).start()
        ag_msg(i, 5).start()
        ag_msg(i, 1, True).wait_recv()
        ag_msg(i, 4).start()
        ag_msg(i, 6).start()

    def ag_h(i):
        ag_msg(i, 3, True).wait_recv()
        ag_msg(i, 7).start()
        ag_msg(i, 4, True).wait_recv()
        ag_msg(i, 8).start()

    def ag_i(i):
        for kind in (2, 5, 6, 7, 8):
            ag_msg(i, kind, True).wait_recv()
        for kind in range(9):
            ag_msg(i, kind).wait_send()

    def out_copy(k, src, dst, layer):
        return pltpu.make_async_copy(src, dst.at[layer], out_sem.at[k])

    def rms(x_val):
        inv = lax.rsqrt(jnp.mean(x_val * x_val, axis=-1, keepdims=True) + EPS)
        return x_val * inv, inv

    barrier = pltpu.get_barrier_semaphore()
    for other in (partner, right, left):
        pl.semaphore_signal(barrier, inc=1, device_id={'tp': other}, device_id_type=MESH)
    loads = [pltpu.make_async_copy(y1_h, part.at[2], in_sem.at[0]),
             pltpu.make_async_copy(dy2_h, part.at[3], in_sem.at[1]),
             pltpu.make_async_copy(blk(y1_h, me), x1.at[1], in_sem.at[2]),
             pltpu.make_async_copy(blk(y2_h, me), x2.at[1], in_sem.at[3]),
             pltpu.make_async_copy(blk(dy1_h, me), dy1, in_sem.at[4]),
             pltpu.make_async_copy(blk(dy2_h, me), dy2, in_sem.at[5])]
    for cp in loads:
        cp.start()
    for cp in w_copies(0):
        cp.start()
    row_id = lax.broadcasted_iota(jnp.int32, (tokens, tokens), 0)
    col_id = lax.broadcasted_iota(jnp.int32, (tokens, tokens), 1)
    seen = jnp.zeros((tokens, tokens), F32)
    for b in range(tp):
        inside = (row_id < (b + 1) * seq) & (col_id >= b * seq) & (col_id <= row_id) & (col_id < b * seq + lens[b])
        seen = jnp.where(inside, 1.0, seen)
    mask[...] = seen
    loads[0].wait()

    @pl.loop(0, tp)
    def _(b):
        r = rows(b * seq)
        n1[r, :] = rms(part[2, r, :])[0].astype(BF16)
    loads[1].wait()

    @pl.loop(0, tp)
    def _(b):
        r = rows(b * seq)
        ee[r, :] = part[3, r, :].astype(BF16)
    for cp in loads[2:]:
        cp.wait()
    pl.semaphore_wait(barrier, 3)

    col_tile = 512

    def product(i, lhs_ref, w_ref):
        @pl.loop(0, width // col_tile)
        def _(j):
            cols = pl.ds(pl.multiple_of(j * col_tile, col_tile), col_tile)
            part[i, :, cols] = mm(lhs_ref[...], w_ref[:, cols], NN)

    @pl.loop(0, n_layers)
    def _(step):
        layer = n_layers - 1 - step
        slot = lax.rem(step, 2)
        other = 1 - slot
        w1_s, w2_s, wqkv_s, wo_s = w1.at[slot], w2.at[slot], wqkv.at[slot], wo.at[slot]
        later = step > 0
        more = step < n_layers - 1
        for cp in w_copies(step):
            cp.wait()

        @pl.when(more)
        def _():
            for cp in w_copies(step + 1):
                cp.start()

        @pl.when(later)
        def _():
            ag_i(2)
        out_copy(0, n1, n1_o, layer).start()
        pre = mm(n1[...], w1_s[...], NT)
        tan = jnp.tanh(GELU_C * (pre + GELU_A * (pre * pre * pre)))
        cdf = 0.5 * (1.0 + tan)
        h_s[...] = (pre * cdf).astype(BF16)
        gp[...] = cdf + pre * (0.5 * GELU_C) * (1.0 - tan * tan) * (1.0 + (3.0 * GELU_A) * (pre * pre))
        out_copy(1, h_s, h_o, layer).start()

        @pl.when(later)
        def _():
            ag_g(3)
        product(0, h_s, w2_s)
        rs_a(0)

        @pl.when(later)
        def _():
            ag_h(3)
        rs_b(0)

        @pl.when(later)
        def _():
            ag_i(3)
        out_copy(2, ee, e_o, layer).start()
        rs_c(0)
        u_s[...] = (gp[...] * mm(ee[...], w2_s[...], NT)).astype(BF16)
        out_copy(3, u_s, u_o, layer).start()
        product(1, u_s, w1_s)
        rs_a(1)
        rs_d(0)
        rs_b(1)
        rs_c(1)
        total = rs_e(0)
        x2_new = x2[other] - total
        x2[slot] = x2_new
        n2[rows(me * seq), :] = rms(x2_new)[0].astype(BF16)
        ag_f(0)
        rs_d(1)
        ag_g(0)
        ag_h(0)
        total = rs_e(1)
        norm, inv = rms(x1[other])
        dy1_new = dy1[...] + inv * (total - norm * jnp.mean(total * norm, axis=-1, keepdims=True))
        dy1[...] = dy1_new
        cc[rows(me * seq), :] = dy1_new.astype(BF16)
        ag_f(1)
        ag_i(0)
        out_copy(4, n2, n2_o, layer).start()
        qkv[...] = mm(n2[...], wqkv_s[...], NT).astype(BF16)
        ag_g(1)
        key, val = qkv[:, qw:qw + hd], qkv[:, qw + hd:qw + 2 * hd]
        for r in range(heads):
            sc = mm(qkv[:, r * hd:(r + 1) * hd], key, NT) * scale
            sc = jnp.where(mask[...] > 0.5, sc, MASK_VALUE)
            ex = jnp.exp(sc - jnp.max(sc, axis=-1, keepdims=True))
            pr = ex / jnp.sum(ex, axis=-1, keepdims=True)
            probs[r] = pr
            att[:, r * hd:(r + 1) * hd] = mm(pr.astype(BF16), val, NN).astype(BF16)
        out_copy(5, att, a_o, layer).start()
        ag_h(1)
        product(2, att, wo_s)
        out_copy(0, n1, n1_o, layer).wait()
        rs_a(2)
        rs_b(2)
        rs_c(2)
        ag_i(1)
        out_copy(6, cc, c_o, layer).start()
        d_att = mm(cc[...], wo_s[...], NT).astype(BF16)
        d_key = jnp.zeros((tokens, hd), F32)
        d_val = jnp.zeros((tokens, hd), F32)
        for r in range(heads):
            da = d_att[:, r * hd:(r + 1) * hd]
            pr = probs[r]
            dp = mm(da, val, NT)
            ds = (pr * (dp - jnp.sum(dp * pr, axis=-1, keepdims=True)) * scale).astype(BF16)
            dqkv[:, r * hd:(r + 1) * hd] = mm(ds, key, NN).astype(BF16)
            d_key = d_key + mm(ds, qkv[:, r * hd:(r + 1) * hd], TN)
            d_val = d_val + mm(pr.astype(BF16), da, TN)
        dqkv[:, qw:qw + hd] = d_key.astype(BF16)
        dqkv[:, qw + hd:qw + 2 * hd] = d_val.astype(BF16)
        out_copy(7, dqkv, d_o, layer).start()
        rs_d(2)
        product(3, dqkv, wqkv_s)
        out_copy(2, ee, e_o, layer).wait()
        rs_a(3)
        rs_b(3)
        rs_c(3)
        total = rs_e(2)
        x1_new = x1[other] - total
        x1[slot] = x1_new
        n1[rows(me * seq), :] = rms(x1_new)[0].astype(BF16)

        @pl.when(more)
        def _():
            ag_f(2)
        rs_d(3)

        @pl.when(more)
        def _():
            ag_g(2)
            ag_h(2)
        total = rs_e(3)
        norm, inv = rms(x2[slot])
        dy2_new = dy2[...] + inv * (total - norm * jnp.mean(total * norm, axis=-1, keepdims=True))
        dy2[...] = dy2_new
        ee[rows(me * seq), :] = dy2_new.astype(BF16)

        @pl.when(more)
        def _():
            ag_f(3)
        for k, src, dst in ((1, h_s, h_o), (3, u_s, u_o), (4, n2, n2_o), (5, att, a_o), (6, cc, c_o), (7, dqkv, d_o)):
            out_copy(k, src, dst, layer).wait()

    last = (n_layers - 1) % 2
    finals = [pltpu.make_async_copy(src, fin_h.at[k], fin_sem.at[k])
              for k, src in enumerate((x1.at[last], x2.at[last], dy1, dy2))]
    for cp in finals:
        cp.start()
    for cp in finals:
        cp.wait()


def solution(mesh):
    tp = mesh.shape['tp']
    assert tp == 8
    act_spec = P('dp', None, None)
    w_specs = (P(None, None, 'tp', None), P(None, None, 'tp', None), P(None, None, 'tp', None),
               P(None, 'tp', None, None), P(None, None, 'tp'), P(None, 'tp', None))
    g_specs = (P('dp', None, 'tp', None), P('dp', None, 'tp', None), P('dp', None, 'tp', None),
               P('dp', 'tp', None, None), P('dp', None, 'tp'), P('dp', 'tp', None))

    def local_fn(y_one, y_two, dy_one, dy_two, seq_lens, w_query, w_key, w_value, w_out, w_up, w_down):
        batch, seq, width = y_one.shape
        n_layers, _, heads, hd = w_query.shape
        assert batch == tp and w_key.shape[2] == 1
        tokens = batch * seq
        ff = w_down.shape[1]
        qw = heads * hd
        half = seq // 2
        acts = [x.reshape(tokens, width) for x in (y_one, y_two, dy_one, dy_two)]

        def flip(w):
            return w.transpose(0, 2, 3, 1).reshape(n_layers, -1, width)
        weights = (w_up.transpose(0, 2, 1), w_down, flip(w_query), flip(w_key), flip(w_value), w_out.reshape(n_layers, qw, width))

        def stack(cols):
            return jax.ShapeDtypeStruct((n_layers, tokens, cols), BF16)
        any_spec = pl.BlockSpec(memory_space=pl.ANY)
        vm = pltpu.VMEM
        dma = pltpu.SemaphoreType.DMA
        scratch = [vm((tokens, width), BF16)] * 4 + [
            vm((2, ff, width), BF16), vm((2, ff, width), BF16), vm((2, qw + 2 * hd, width), BF16), vm((2, qw, width), BF16),
            vm((tokens, ff), BF16), vm((tokens, ff), BF16), vm((tokens, ff), F32),
            vm((tokens, qw + 2 * hd), BF16), vm((tokens, qw), BF16), vm((tokens, qw + 2 * hd), BF16),
            vm((heads, tokens, tokens), F32), vm((tokens, tokens), F32),
            vm((2, seq, width), F32), vm((2, seq, width), F32), vm((seq, width), F32), vm((seq, width), F32),
            vm((4, tokens, width), F32), vm((4, 4, seq, width), F32), vm((4, 2, half, width), F32), vm((4, 2, seq, width), F32),
            dma((2, 6)), dma((6,)), dma((8,)), dma((4,)), dma((4, 10)), dma((4, 10)), dma((4, 9)), dma((4, 9))]
        fin, n1, n2, c_val, e_val, h_val, u_val, a_val, d_val = pl.pallas_call(
            functools.partial(chain_kernel, (n_layers, tp, seq, width, heads, hd)),
            out_shape=(jax.ShapeDtypeStruct((4, seq, width), F32), stack(width), stack(width), stack(width), stack(width),
                       stack(ff), stack(ff), stack(qw), stack(qw + 2 * hd)),
            in_specs=[pl.BlockSpec(memory_space=pltpu.SMEM)] + [any_spec] * 10,
            out_specs=(any_spec,) * 9,
            scratch_shapes=scratch,
            compiler_params=pltpu.CompilerParams(collective_id=0, has_side_effects=True, vmem_limit_bytes=66_000_000),
            name='chain',
        )(seq_lens, *acts, *weights)

        def grad(small, wide):
            return jnp.einsum('lts,ltd->lsd', small, wide, preferred_element_type=F32)
        dw_up = grad(u_val, n1).transpose(0, 2, 1)
        dw_down = grad(h_val, e_val)
        dw_out = grad(a_val, c_val).reshape(w_out.shape)

        def flip_back(g, like):
            return g.reshape(n_layers, -1, hd, width).transpose(0, 3, 1, 2).reshape(like.shape)
        dw_query = flip_back(grad(d_val[:, :, :qw], n2), w_query)
        dw_key = flip_back(grad(d_val[:, :, qw:qw + hd], n2), w_key)
        dw_value = flip_back(grad(d_val[:, :, qw + hd:], n2), w_value)
        ends = tuple(lax.all_gather(fin[k:k + 1], 'tp', axis=0, tiled=True) for k in range(4))
        return ends + (dw_query, dw_key, dw_value, dw_out, dw_up, dw_down)

    return jax.shard_map(local_fn, mesh=mesh,
                         in_specs=(act_spec,) * 4 + (P('dp'),) + w_specs,
                         out_specs=(act_spec,) * 4 + g_specs,
                         check_vma=False)
```

```python
import functools

import jax
import jax.numpy as jnp
from jax import lax
from jax.experimental import pallas as pl
from jax.experimental.pallas import tpu as pltpu
from jax.sharding import PartitionSpec as P

F32 = jnp.float32
BF16 = jnp.bfloat16
EPS = 1e-5
MASK_VALUE = -1e30
GELU_C = 0.7978845608028654
GELU_A = 0.044715
MESH = pl.DeviceIdType.MESH
NT = (((1,), (1,)), ((), ()))
NN = (((1,), (0,)), ((), ()))
TN = (((0,), (0,)), ((), ()))


def mm(lhs, rhs, dims):
    return lax.dot_general(lhs, rhs, dims, preferred_element_type=F32)


def chain_kernel(cfg, lens, y1_h, y2_h, dy1_h, dy2_h, w1_h, w2_h, wq_h, wk_h, wv_h, wo_h,
                 f_x1, f_x2, f_dy1, f_dy2, n1_o, n2_o, c_o, e_o, h_o, u_o, a_o, d_o,
                 n1, n2, cc, ee, w1, w2, wqkv, wo, h_s, u_s, gp, qkv, att, dqkv, probs, mask,
                 x1, x2, dy1, dy2, part, ra, rb, rc, fbuf,
                 w_sem, in_sem, out_sem, fin_sem, rs_send, rs_recv, ag_send, ag_recv):
    n_layers, tp, seq, width, heads, hd = cfg
    chips = tp // 2
    tokens = tp * seq
    half = seq // 2
    scale = hd ** -0.5
    qw = heads * hd
    me = lax.axis_index('tp')
    chip = me // 2
    core = me - 2 * chip
    partner = me + 1 - 2 * core
    right = lax.rem(me + 2, tp)
    left = lax.rem(me + tp - 2, tp)
    opp = lax.rem(me + chips, tp)

    def rows(start, size=seq):
        return pl.ds(pl.multiple_of(start, half), size)

    def blk(ref, who):
        return ref.at[rows(who * seq)]

    def blk_a(ref, who):
        return ref.at[rows(who * seq, half)]

    def blk_b(ref, who):
        return ref.at[rows(who * seq + half, half)]

    def rcopy(src, dst, send, recv, dev):
        return pltpu.make_async_remote_copy(src_ref=src, dst_ref=dst, send_sem=send, recv_sem=recv,
                                            device_id={'tp': dev}, device_id_type=MESH)

    def w_copies(step):
        layer = n_layers - 1 - step
        slot = lax.rem(step, 2)
        kw = wk_h.shape[1]
        return (pltpu.make_async_copy(w1_h.at[layer], w1.at[slot], w_sem.at[slot, 0]),
                pltpu.make_async_copy(w2_h.at[layer], w2.at[slot], w_sem.at[slot, 1]),
                pltpu.make_async_copy(wq_h.at[layer], wqkv.at[slot, pl.ds(0, qw)], w_sem.at[slot, 2]),
                pltpu.make_async_copy(wk_h.at[layer], wqkv.at[slot, pl.ds(qw, kw)], w_sem.at[slot, 3]),
                pltpu.make_async_copy(wv_h.at[layer], wqkv.at[slot, pl.ds(qw + kw, kw)], w_sem.at[slot, 4]),
                pltpu.make_async_copy(wo_h.at[layer], wo.at[slot], w_sem.at[slot, 5]))

    owners = (opp, right, left, me)

    def rs_d2d(i, role):
        own = owners[role]
        theirs = own + 1 - 2 * core
        return rcopy(blk(part.at[i], theirs), ra.at[i, role], rs_send.at[i, role], rs_recv.at[i, role], partner)

    def rs_ring(i, kind):
        pt = part.at[i]
        lo, hi = pl.ds(0, half), pl.ds(half, half)
        src, dst, dev = ((blk_a(pt, opp), rb.at[i, 0], right), (blk_b(pt, opp), rb.at[i, 1], left),
                         (blk_b(pt, right), rc.at[i, 0, hi], right), (blk_a(pt, left), rc.at[i, 1, lo], left),
                         (blk_a(pt, right), rc.at[i, 0, lo], right), (blk_b(pt, left), rc.at[i, 1, hi], left))[kind]
        return rcopy(src, dst, rs_send.at[i, 4 + kind], rs_recv.at[i, 4 + kind], dev)

    def rs_add(i, who, extra, off=0, size=seq):
        where_rows = rows(who * seq + off, size)
        part[i, where_rows, :] = part[i, where_rows, :] + extra

    def rs_a(i):
        for role in range(4):
            rs_d2d(i, role).start()

    def rs_b(i):
        rs_d2d(i, 0).wait_recv()
        rs_add(i, opp, ra[i, 0])
        rs_ring(i, 0).start()
        rs_ring(i, 1).start()

    def rs_c(i):
        rs_d2d(i, 1).wait_recv()
        rs_add(i, right, ra[i, 1])
        rs_ring(i, 2).start()
        rs_d2d(i, 2).wait_recv()
        rs_add(i, left, ra[i, 2])
        rs_ring(i, 3).start()

    def rs_d(i):
        rs_ring(i, 0).wait_recv()
        rs_add(i, right, rb[i, 0], 0, half)
        rs_ring(i, 4).start()
        rs_ring(i, 1).wait_recv()
        rs_add(i, left, rb[i, 1], half, half)
        rs_ring(i, 5).start()

    def rs_e(i):
        rs_d2d(i, 3).wait_recv()
        for kind in range(2, 6):
            rs_ring(i, kind).wait_recv()
        for role in range(4):
            rs_d2d(i, role).wait_send()
        for kind in range(6):
            rs_ring(i, kind).wait_send()
        return (part[i, rows(me * seq), :] + ra[i, 3]) + (rc[i, 0] + rc[i, 1])

    bufs = (n2, cc, n1, ee, fbuf.at[0], fbuf.at[1], fbuf.at[2], fbuf.at[3])
    f_out = (f_x1, f_x2, f_dy1, f_dy2)

    def ag_msg(i, kind, receive=False):
        buf = bufs[i]
        if receive:
            p_left = lax.rem(partner + tp - 2, tp)
            p_right = lax.rem(partner + 2, tp)
            p_opp = lax.rem(partner + chips, tp)
            ref = (lambda: blk(buf, left), lambda: blk(buf, right), lambda: blk(buf, partner), lambda: blk_a(buf, opp),
                   lambda: blk_b(buf, opp), lambda: blk(buf, p_left), lambda: blk(buf, p_right),
                   lambda: blk_a(buf, p_opp), lambda: blk_b(buf, p_opp))[kind]()
        else:
            ref = (lambda: blk(buf, me), lambda: blk(buf, me), lambda: blk(buf, me), lambda: blk_a(buf, left),
                   lambda: blk_b(buf, right), lambda: blk(buf, left), lambda: blk(buf, right),
                   lambda: blk_a(buf, opp), lambda: blk_b(buf, opp))[kind]()
        dev = (right, left, partner, right, left, partner, partner, partner, partner)[kind]
        return rcopy(ref, ref, ag_send.at[i, kind], ag_recv.at[i, kind], dev)

    def ag_f(i):
        for kind in range(3):
            ag_msg(i, kind).start()

    def ag_g(i):
        ag_msg(i, 0, True).wait_recv()
        ag_msg(i, 3).start()
        ag_msg(i, 5).start()
        ag_msg(i, 1, True).wait_recv()
        ag_msg(i, 4).start()
        ag_msg(i, 6).start()

    def ag_h(i):
        ag_msg(i, 3, True).wait_recv()
        ag_msg(i, 7).start()
        ag_msg(i, 4, True).wait_recv()
        ag_msg(i, 8).start()

    def ag_i(i):
        for kind in (2, 5, 6, 7, 8):
            ag_msg(i, kind, True).wait_recv()
        for kind in range(9):
            ag_msg(i, kind).wait_send()

    def fin_start(k, value):
        fbuf[k, rows(me * seq), :] = value
        ag_f(4 + k)

    def fin_copy(k):
        return pltpu.make_async_copy(fbuf.at[k], f_out[k], fin_sem.at[k])

    def fin_end(k):
        ag_i(4 + k)
        fin_copy(k).start()

    def out_copy(k, src, dst, layer):
        return pltpu.make_async_copy(src, dst.at[layer], out_sem.at[k])

    def rms(x_val):
        inv = lax.rsqrt(jnp.mean(x_val * x_val, axis=-1, keepdims=True) + EPS)
        return x_val * inv, inv

    barrier = pltpu.get_barrier_semaphore()
    for other in (partner, right, left):
        pl.semaphore_signal(barrier, inc=1, device_id={'tp': other}, device_id_type=MESH)
    loads = [pltpu.make_async_copy(y1_h, part.at[2], in_sem.at[0]),
             pltpu.make_async_copy(dy2_h, part.at[3], in_sem.at[1]),
             pltpu.make_async_copy(blk(y1_h, me), x1.at[1], in_sem.at[2]),
             pltpu.make_async_copy(blk(y2_h, me), x2.at[1], in_sem.at[3]),
             pltpu.make_async_copy(blk(dy1_h, me), dy1, in_sem.at[4]),
             pltpu.make_async_copy(blk(dy2_h, me), dy2, in_sem.at[5])]
    for cp in loads:
        cp.start()
    for cp in w_copies(0):
        cp.start()
    row_id = lax.broadcasted_iota(jnp.int32, (tokens, tokens), 0)
    col_id = lax.broadcasted_iota(jnp.int32, (tokens, tokens), 1)
    seen = jnp.zeros((tokens, tokens), F32)
    for b in range(tp):
        inside = (row_id < (b + 1) * seq) & (col_id >= b * seq) & (col_id <= row_id) & (col_id < b * seq + lens[b])
        seen = jnp.where(inside, 1.0, seen)
    mask[...] = seen
    loads[0].wait()

    @pl.loop(0, tp)
    def _(b):
        r = rows(b * seq)
        n1[r, :] = rms(part[2, r, :])[0].astype(BF16)
    loads[1].wait()

    @pl.loop(0, tp)
    def _(b):
        r = rows(b * seq)
        ee[r, :] = part[3, r, :].astype(BF16)
    for cp in loads[2:]:
        cp.wait()
    pl.semaphore_wait(barrier, 3)

    col_tile = 512

    def product(i, lhs_ref, w_ref):
        @pl.loop(0, width // col_tile)
        def _(j):
            cols = pl.ds(pl.multiple_of(j * col_tile, col_tile), col_tile)
            part[i, :, cols] = mm(lhs_ref[...], w_ref[:, cols], NN)

    @pl.loop(0, n_layers)
    def _(step):
        layer = n_layers - 1 - step
        slot = lax.rem(step, 2)
        other = 1 - slot
        w1_s, w2_s, wqkv_s, wo_s = w1.at[slot], w2.at[slot], wqkv.at[slot], wo.at[slot]
        later = step > 0
        more = step < n_layers - 1
        end = step == n_layers - 1
        for cp in w_copies(step):
            cp.wait()

        @pl.when(more)
        def _():
            for cp in w_copies(step + 1):
                cp.start()

        @pl.when(later)
        def _():
            ag_i(2)
        out_copy(0, n1, n1_o, layer).start()
        pre = mm(n1[...], w1_s[...], NT)
        tan = jnp.tanh(GELU_C * (pre + GELU_A * (pre * pre * pre)))
        cdf = 0.5 * (1.0 + tan)
        h_s[...] = (pre * cdf).astype(BF16)
        gp[...] = cdf + pre * (0.5 * GELU_C) * (1.0 - tan * tan) * (1.0 + (3.0 * GELU_A) * (pre * pre))
        out_copy(1, h_s, h_o, layer).start()

        @pl.when(later)
        def _():
            ag_g(3)
        product(0, h_s, w2_s)
        rs_a(0)

        @pl.when(later)
        def _():
            ag_h(3)
        rs_b(0)

        @pl.when(later)
        def _():
            ag_i(3)
        out_copy(2, ee, e_o, layer).start()
        rs_c(0)
        u_s[...] = (gp[...] * mm(ee[...], w2_s[...], NT)).astype(BF16)
        out_copy(3, u_s, u_o, layer).start()
        product(1, u_s, w1_s)
        rs_a(1)
        rs_d(0)
        rs_b(1)
        rs_c(1)
        total = rs_e(0)
        x2_new = x2[other] - total
        x2[slot] = x2_new
        n2[rows(me * seq), :] = rms(x2_new)[0].astype(BF16)
        ag_f(0)
        rs_d(1)
        ag_g(0)
        ag_h(0)
        total = rs_e(1)
        norm, inv = rms(x1[other])
        dy1_new = dy1[...] + inv * (total - norm * jnp.mean(total * norm, axis=-1, keepdims=True))
        dy1[...] = dy1_new
        cc[rows(me * seq), :] = dy1_new.astype(BF16)
        ag_f(1)
        ag_i(0)
        out_copy(4, n2, n2_o, layer).start()
        qkv[...] = mm(n2[...], wqkv_s[...], NT).astype(BF16)
        ag_g(1)
        key, val = qkv[:, qw:qw + hd], qkv[:, qw + hd:qw + 2 * hd]
        for r in range(heads):
            sc = mm(qkv[:, r * hd:(r + 1) * hd], key, NT) * scale
            sc = jnp.where(mask[...] > 0.5, sc, MASK_VALUE)
            ex = jnp.exp(sc - jnp.max(sc, axis=-1, keepdims=True))
            pr = ex / jnp.sum(ex, axis=-1, keepdims=True)
            probs[r] = pr
            att[:, r * hd:(r + 1) * hd] = mm(pr.astype(BF16), val, NN).astype(BF16)
        out_copy(5, att, a_o, layer).start()
        ag_h(1)

        @pl.when(end)
        def _():
            fin_start(1, x2[slot])
        product(2, att, wo_s)
        out_copy(0, n1, n1_o, layer).wait()
        rs_a(2)
        rs_b(2)

        @pl.when(end)
        def _():
            ag_g(5)
        rs_c(2)
        ag_i(1)

        @pl.when(end)
        def _():
            fin_start(2, dy1[...])
        out_copy(6, cc, c_o, layer).start()
        d_att = mm(cc[...], wo_s[...], NT).astype(BF16)
        d_key = jnp.zeros((tokens, hd), F32)
        d_val = jnp.zeros((tokens, hd), F32)
        for r in range(heads):
            da = d_att[:, r * hd:(r + 1) * hd]
            pr = probs[r]
            dp = mm(da, val, NT)
            ds = (pr * (dp - jnp.sum(dp * pr, axis=-1, keepdims=True)) * scale).astype(BF16)
            dqkv[:, r * hd:(r + 1) * hd] = mm(ds, key, NN).astype(BF16)
            d_key = d_key + mm(ds, qkv[:, r * hd:(r + 1) * hd], TN)
            d_val = d_val + mm(pr.astype(BF16), da, TN)
        dqkv[:, qw:qw + hd] = d_key.astype(BF16)
        dqkv[:, qw + hd:qw + 2 * hd] = d_val.astype(BF16)
        out_copy(7, dqkv, d_o, layer).start()
        rs_d(2)

        @pl.when(end)
        def _():
            ag_h(5)
            ag_g(6)
        product(3, dqkv, wqkv_s)
        out_copy(2, ee, e_o, layer).wait()
        rs_a(3)
        rs_b(3)
        rs_c(3)

        @pl.when(end)
        def _():
            ag_h(6)
        total = rs_e(2)
        x1_new = x1[other] - total
        x1[slot] = x1_new
        n1[rows(me * seq), :] = rms(x1_new)[0].astype(BF16)

        @pl.when(more)
        def _():
            ag_f(2)

        @pl.when(end)
        def _():
            fin_start(0, x1_new)
        rs_d(3)

        @pl.when(more)
        def _():
            ag_g(2)
            ag_h(2)

        @pl.when(end)
        def _():
            fin_end(1)
            fin_end(2)
            ag_g(4)
            ag_h(4)
        total = rs_e(3)
        norm, inv = rms(x2[slot])
        dy2_new = dy2[...] + inv * (total - norm * jnp.mean(total * norm, axis=-1, keepdims=True))
        dy2[...] = dy2_new
        ee[rows(me * seq), :] = dy2_new.astype(BF16)

        @pl.when(more)
        def _():
            ag_f(3)

        @pl.when(end)
        def _():
            fin_start(3, dy2_new)
        for k, src, dst in ((1, h_s, h_o), (3, u_s, u_o), (4, n2, n2_o), (5, att, a_o), (6, cc, c_o), (7, dqkv, d_o)):
            out_copy(k, src, dst, layer).wait()

    ag_g(7)
    ag_h(7)
    fin_end(0)
    fin_end(3)
    for k in range(4):
        fin_copy(k).wait()


def grad_kernel(parts, n1, n2, c_val, e_val, h_val, u_val, a_val, d_val, g_up, g_down, g_q, g_k, g_v, g_out):
    qw, hd = parts
    g_up[0] = mm(u_val[0], n1[0], TN)
    g_down[0] = mm(h_val[0], e_val[0], TN)
    g_out[0] = mm(a_val[0], c_val[0], TN)
    g_all = mm(d_val[0], n2[0], TN)
    g_q[0] = g_all[:qw]
    g_k[0] = g_all[qw:qw + hd]
    g_v[0] = g_all[qw + hd:]


def solution(mesh):
    tp = mesh.shape['tp']
    assert tp == 8
    act_spec = P('dp', None, None)
    w_specs = (P(None, None, 'tp', None), P(None, None, 'tp', None), P(None, None, 'tp', None),
               P(None, 'tp', None, None), P(None, None, 'tp'), P(None, 'tp', None))
    g_specs = (P('dp', None, 'tp', None), P('dp', None, 'tp', None), P('dp', None, 'tp', None),
               P('dp', 'tp', None, None), P('dp', None, 'tp'), P('dp', 'tp', None))

    def local_fn(y_one, y_two, dy_one, dy_two, seq_lens, w_query, w_key, w_value, w_out, w_up, w_down):
        batch, seq, width = y_one.shape
        n_layers, _, heads, hd = w_query.shape
        assert batch == tp and w_key.shape[2] == 1
        tokens = batch * seq
        ff = w_down.shape[1]
        qw = heads * hd
        half = seq // 2
        acts = [x.reshape(tokens, width) for x in (y_one, y_two, dy_one, dy_two)]

        def flip(w):
            return w.transpose(0, 2, 3, 1).reshape(n_layers, -1, width)
        weights = (w_up.transpose(0, 2, 1), w_down, flip(w_query), flip(w_key), flip(w_value), w_out.reshape(n_layers, qw, width))

        def stack(cols):
            return jax.ShapeDtypeStruct((n_layers, tokens, cols), BF16)
        any_spec = pl.BlockSpec(memory_space=pl.ANY)
        vm = pltpu.VMEM
        dma = pltpu.SemaphoreType.DMA
        scratch = [vm((tokens, width), BF16)] * 4 + [
            vm((2, ff, width), BF16), vm((2, ff, width), BF16), vm((2, qw + 2 * hd, width), BF16), vm((2, qw, width), BF16),
            vm((tokens, ff), BF16), vm((tokens, ff), BF16), vm((tokens, ff), F32),
            vm((tokens, qw + 2 * hd), BF16), vm((tokens, qw), BF16), vm((tokens, qw + 2 * hd), BF16),
            vm((heads, tokens, tokens), F32), vm((tokens, tokens), F32),
            vm((2, seq, width), F32), vm((2, seq, width), F32), vm((seq, width), F32), vm((seq, width), F32),
            vm((4, tokens, width), F32), vm((4, 4, seq, width), F32), vm((4, 2, half, width), F32), vm((4, 2, seq, width), F32),
            vm((4, tokens, width), F32),
            dma((2, 6)), dma((6,)), dma((8,)), dma((4,)), dma((4, 10)), dma((4, 10)), dma((8, 9)), dma((8, 9))]
        *ends, n1, n2, c_val, e_val, h_val, u_val, a_val, d_val = pl.pallas_call(
            functools.partial(chain_kernel, (n_layers, tp, seq, width, heads, hd)),
            out_shape=(jax.ShapeDtypeStruct((tokens, width), F32),) * 4 + (stack(width), stack(width), stack(width), stack(width),
                       stack(ff), stack(ff), stack(qw), stack(qw + 2 * hd)),
            in_specs=[pl.BlockSpec(memory_space=pltpu.SMEM)] + [any_spec] * 10,
            out_specs=(any_spec,) * 12,
            scratch_shapes=scratch,
            compiler_params=pltpu.CompilerParams(collective_id=0, has_side_effects=True, vmem_limit_bytes=66_000_000),
            name='chain',
        )(seq_lens, *acts, *weights)

        col_tile = 512

        def wide():
            return pl.BlockSpec((1, tokens, col_tile), lambda layer, j: (layer, 0, j))

        def small(cols):
            return pl.BlockSpec((1, tokens, cols), lambda layer, j: (layer, 0, 0))
        g_rows = (ff, ff, qw, hd, hd, qw)
        moved = 2 * n_layers * tokens * (4 * width + 2 * ff + 2 * qw + 2 * hd) + 4 * n_layers * width * sum(g_rows)
        g_up, g_down, g_q, g_k, g_v, g_out = pl.pallas_call(
            functools.partial(grad_kernel, (qw, hd)),
            grid=(n_layers, width // col_tile),
            out_shape=tuple(jax.ShapeDtypeStruct((n_layers, r, width), F32) for r in g_rows),
            in_specs=[wide()] * 4 + [small(ff), small(ff), small(qw), small(qw + 2 * hd)],
            out_specs=tuple(pl.BlockSpec((1, r, col_tile), lambda layer, j: (layer, 0, j)) for r in g_rows),
            compiler_params=pltpu.CompilerParams(vmem_limit_bytes=60_000_000),
            cost_estimate=pl.CostEstimate(flops=2 * n_layers * tokens * width * sum(g_rows), bytes_accessed=moved, transcendentals=0),
            name='grads',
        )(n1, n2, c_val, e_val, h_val, u_val, a_val, d_val)

        def flip_back(g, like):
            return g.reshape(n_layers, -1, hd, width).transpose(0, 3, 1, 2).reshape(like.shape)
        dw_up, dw_down, dw_out = g_up.transpose(0, 2, 1), g_down, g_out.reshape(w_out.shape)
        dw_query, dw_key, dw_value = flip_back(g_q, w_query), flip_back(g_k, w_key), flip_back(g_v, w_value)
        ends = tuple(v.reshape(batch, seq, width) for v in ends)
        return ends + (dw_query, dw_key, dw_value, dw_out, dw_up, dw_down)

    return jax.shard_map(local_fn, mesh=mesh,
                         in_specs=(act_spec,) * 4 + (P('dp'),) + w_specs,
                         out_specs=(act_spec,) * 4 + g_specs,
                         check_vma=False)
```

```python
import functools

import jax
import jax.numpy as jnp
from jax import lax
from jax.experimental import pallas as pl
from jax.experimental.pallas import tpu as pltpu
from jax.sharding import PartitionSpec as P

F32 = jnp.float32
BF16 = jnp.bfloat16
EPS = 1e-5
MASK_VALUE = -1e30
GELU_C = 0.7978845608028654
GELU_A = 0.044715
MESH = pl.DeviceIdType.MESH
NT = (((1,), (1,)), ((), ()))
NN = (((1,), (0,)), ((), ()))
TN = (((0,), (0,)), ((), ()))


def mm(lhs, rhs, dims):
    return lax.dot_general(lhs, rhs, dims, preferred_element_type=F32)


def chain_kernel(cfg, lens, y1_h, y2_h, dy1_h, dy2_h, w1_h, w2_h, wq_h, wk_h, wv_h, wo_h,
                 f_x1, f_x2, f_dy1, f_dy2, n1_o, n2_o, c_o, e_o, h_o, u_o, a_o, d_o,
                 n1, n2, cc, ee, w1, w2, wqkv, wo, h_s, u_s, gp, qkv, att, dqkv, probs, mask,
                 x1, x2, dy1, dy2, part, ra, rb, rc, fbuf,
                 w_sem, in_sem, out_sem, fin_sem, rs_send, rs_recv, ag_send, ag_recv):
    n_layers, tp, seq, width, heads, hd = cfg
    chips = tp // 2
    tokens = tp * seq
    half = seq // 2
    scale = hd ** -0.5
    qw = heads * hd
    me = lax.axis_index('tp')
    chip = me // 2
    core = me - 2 * chip
    partner = me + 1 - 2 * core
    right = lax.rem(me + 2, tp)
    left = lax.rem(me + tp - 2, tp)
    opp = lax.rem(me + chips, tp)

    def rows(start, size=seq):
        return pl.ds(pl.multiple_of(start, half), size)

    def blk(ref, who):
        return ref.at[rows(who * seq)]

    def blk_a(ref, who):
        return ref.at[rows(who * seq, half)]

    def blk_b(ref, who):
        return ref.at[rows(who * seq + half, half)]

    def rcopy(src, dst, send, recv, dev):
        return pltpu.make_async_remote_copy(src_ref=src, dst_ref=dst, send_sem=send, recv_sem=recv,
                                            device_id={'tp': dev}, device_id_type=MESH)

    def w_copies(step):
        layer = n_layers - 1 - step
        slot = lax.rem(step, 2)
        kw = wk_h.shape[1]
        return (pltpu.make_async_copy(w1_h.at[layer], w1.at[slot], w_sem.at[slot, 0]),
                pltpu.make_async_copy(w2_h.at[layer], w2.at[slot], w_sem.at[slot, 1]),
                pltpu.make_async_copy(wq_h.at[layer], wqkv.at[slot, pl.ds(0, qw)], w_sem.at[slot, 2]),
                pltpu.make_async_copy(wk_h.at[layer], wqkv.at[slot, pl.ds(qw, kw)], w_sem.at[slot, 3]),
                pltpu.make_async_copy(wv_h.at[layer], wqkv.at[slot, pl.ds(qw + kw, kw)], w_sem.at[slot, 4]),
                pltpu.make_async_copy(wo_h.at[layer], wo.at[slot], w_sem.at[slot, 5]))

    owners = (opp, right, left, me)

    def rs_d2d(i, role):
        own = owners[role]
        theirs = own + 1 - 2 * core
        return rcopy(blk(part.at[i], theirs), ra.at[i, role], rs_send.at[i, role], rs_recv.at[i, role], partner)

    def rs_ring(i, kind):
        pt = part.at[i]
        lo, hi = pl.ds(0, half), pl.ds(half, half)
        src, dst, dev = ((blk_a(pt, opp), rb.at[i, 0], right), (blk_b(pt, opp), rb.at[i, 1], left),
                         (blk_b(pt, right), rc.at[i, 0, hi], right), (blk_a(pt, left), rc.at[i, 1, lo], left),
                         (blk_a(pt, right), rc.at[i, 0, lo], right), (blk_b(pt, left), rc.at[i, 1, hi], left))[kind]
        return rcopy(src, dst, rs_send.at[i, 4 + kind], rs_recv.at[i, 4 + kind], dev)

    def rs_add(i, who, extra, off=0, size=seq):
        where_rows = rows(who * seq + off, size)
        part[i, where_rows, :] = part[i, where_rows, :] + extra

    def rs_a(i):
        for role in range(4):
            rs_d2d(i, role).start()

    def rs_b(i):
        rs_d2d(i, 0).wait_recv()
        rs_add(i, opp, ra[i, 0])
        rs_ring(i, 0).start()
        rs_ring(i, 1).start()

    def rs_c(i):
        rs_d2d(i, 1).wait_recv()
        rs_add(i, right, ra[i, 1])
        rs_ring(i, 2).start()
        rs_d2d(i, 2).wait_recv()
        rs_add(i, left, ra[i, 2])
        rs_ring(i, 3).start()

    def rs_d(i):
        rs_ring(i, 0).wait_recv()
        rs_add(i, right, rb[i, 0], 0, half)
        rs_ring(i, 4).start()
        rs_ring(i, 1).wait_recv()
        rs_add(i, left, rb[i, 1], half, half)
        rs_ring(i, 5).start()

    def rs_e(i):
        rs_d2d(i, 3).wait_recv()
        for kind in range(2, 6):
            rs_ring(i, kind).wait_recv()
        for role in range(4):
            rs_d2d(i, role).wait_send()
        for kind in range(6):
            rs_ring(i, kind).wait_send()
        return (part[i, rows(me * seq), :] + ra[i, 3]) + (rc[i, 0] + rc[i, 1])

    bufs = (n2, cc, n1, ee, fbuf.at[0], fbuf.at[1], fbuf.at[2], fbuf.at[3])
    f_out = (f_x1, f_x2, f_dy1, f_dy2)

    def ag_msg(i, kind, receive=False):
        buf = bufs[i]
        if receive:
            p_left = lax.rem(partner + tp - 2, tp)
            p_right = lax.rem(partner + 2, tp)
            p_opp = lax.rem(partner + chips, tp)
            ref = (lambda: blk(buf, left), lambda: blk(buf, right), lambda: blk(buf, partner), lambda: blk_a(buf, opp),
                   lambda: blk_b(buf, opp), lambda: blk(buf, p_left), lambda: blk(buf, p_right),
                   lambda: blk_a(buf, p_opp), lambda: blk_b(buf, p_opp))[kind]()
        else:
            ref = (lambda: blk(buf, me), lambda: blk(buf, me), lambda: blk(buf, me), lambda: blk_a(buf, left),
                   lambda: blk_b(buf, right), lambda: blk(buf, left), lambda: blk(buf, right),
                   lambda: blk_a(buf, opp), lambda: blk_b(buf, opp))[kind]()
        dev = (right, left, partner, right, left, partner, partner, partner, partner)[kind]
        return rcopy(ref, ref, ag_send.at[i, kind], ag_recv.at[i, kind], dev)

    def ag_f(i):
        for kind in range(3):
            ag_msg(i, kind).start()

    def ag_g(i):
        ag_msg(i, 0, True).wait_recv()
        ag_msg(i, 3).start()
        ag_msg(i, 5).start()
        ag_msg(i, 1, True).wait_recv()
        ag_msg(i, 4).start()
        ag_msg(i, 6).start()

    def ag_h(i):
        ag_msg(i, 3, True).wait_recv()
        ag_msg(i, 7).start()
        ag_msg(i, 4, True).wait_recv()
        ag_msg(i, 8).start()

    def ag_i(i):
        for kind in (2, 5, 6, 7, 8):
            ag_msg(i, kind, True).wait_recv()
        for kind in range(9):
            ag_msg(i, kind).wait_send()

    def fin_start(k, value):
        fbuf[k, rows(me * seq), :] = value
        ag_f(4 + k)

    def fin_copy(k):
        return pltpu.make_async_copy(fbuf.at[k], f_out[k], fin_sem.at[k])

    def fin_end(k):
        ag_i(4 + k)
        fin_copy(k).start()

    def out_copy(k, src, dst, layer):
        return pltpu.make_async_copy(src, dst.at[layer], out_sem.at[k])

    def rms(x_val):
        inv = lax.rsqrt(jnp.mean(x_val * x_val, axis=-1, keepdims=True) + EPS)
        return x_val * inv, inv

    barrier = pltpu.get_barrier_semaphore()
    for other in (partner, right, left):
        pl.semaphore_signal(barrier, inc=1, device_id={'tp': other}, device_id_type=MESH)
    loads = [pltpu.make_async_copy(y1_h, part.at[2], in_sem.at[0]),
             pltpu.make_async_copy(dy2_h, part.at[3], in_sem.at[1]),
             pltpu.make_async_copy(blk(y1_h, me), x1.at[1], in_sem.at[2]),
             pltpu.make_async_copy(blk(y2_h, me), x2.at[1], in_sem.at[3]),
             pltpu.make_async_copy(blk(dy1_h, me), dy1, in_sem.at[4]),
             pltpu.make_async_copy(blk(dy2_h, me), dy2, in_sem.at[5])]
    first = w_copies(0)
    for cp in (loads[0], first[0], loads[1], first[1], *loads[2:], *first[2:]):
        cp.start()
    loads[0].wait()

    @pl.loop(0, tp)
    def _(b):
        r = rows(b * seq)
        n1[r, :] = rms(part[2, r, :])[0].astype(BF16)
    pl.semaphore_wait(barrier, 3)

    col_tile = 512

    def product(i, lhs_ref, w_ref):
        @pl.loop(0, width // col_tile)
        def _(j):
            cols = pl.ds(pl.multiple_of(j * col_tile, col_tile), col_tile)
            part[i, :, cols] = mm(lhs_ref[...], w_ref[:, cols], NN)

    @pl.loop(0, n_layers)
    def _(step):
        layer = n_layers - 1 - step
        slot = lax.rem(step, 2)
        other = 1 - slot
        w1_s, w2_s, wqkv_s, wo_s = w1.at[slot], w2.at[slot], wqkv.at[slot], wo.at[slot]
        later = step > 0
        more = step < n_layers - 1
        end = step == n_layers - 1
        now = w_copies(step)
        now[0].wait()

        @pl.when(more)
        def _():
            for cp in w_copies(step + 1):
                cp.start()

        @pl.when(later)
        def _():
            ag_i(2)
        out_copy(0, n1, n1_o, layer).start()
        pre = mm(n1[...], w1_s[...], NT)
        tan = jnp.tanh(GELU_C * (pre + GELU_A * (pre * pre * pre)))
        cdf = 0.5 * (1.0 + tan)
        h_s[...] = (pre * cdf).astype(BF16)
        gp[...] = cdf + pre * (0.5 * GELU_C) * (1.0 - tan * tan) * (1.0 + (3.0 * GELU_A) * (pre * pre))
        out_copy(1, h_s, h_o, layer).start()

        @pl.when(later)
        def _():
            total = rs_e(3)
            norm, inv = rms(x2[other])
            dy2_new = dy2[...] + inv * (total - norm * jnp.mean(total * norm, axis=-1, keepdims=True))
            dy2[...] = dy2_new
            ee[rows(me * seq), :] = dy2_new.astype(BF16)
            ag_f(3)
        now[1].wait()
        product(0, h_s, w2_s)
        rs_a(0)

        @pl.when(step == 0)
        def _():
            loads[1].wait()

            @pl.loop(0, tp)
            def _(b):
                r = rows(b * seq)
                ee[r, :] = part[3, r, :].astype(BF16)
        rs_b(0)

        @pl.when(later)
        def _():
            ag_g(3)
        rs_c(0)
        rs_d(0)

        @pl.when(step == 0)
        def _():
            row_id = lax.broadcasted_iota(jnp.int32, (tokens, tokens), 0)
            col_id = lax.broadcasted_iota(jnp.int32, (tokens, tokens), 1)
            seen = jnp.zeros((tokens, tokens), F32)
            for b in range(tp):
                inside = (row_id < (b + 1) * seq) & (col_id >= b * seq) & (col_id <= row_id) & (col_id < b * seq + lens[b])
                seen = jnp.where(inside, 1.0, seen)
            mask[...] = seen
            for cp in loads[2:]:
                cp.wait()

        @pl.when(later)
        def _():
            ag_h(3)
            ag_i(3)
        out_copy(2, ee, e_o, layer).start()
        u_s[...] = (gp[...] * mm(ee[...], w2_s[...], NT)).astype(BF16)
        out_copy(3, u_s, u_o, layer).start()
        product(1, u_s, w1_s)
        rs_a(1)
        rs_b(1)
        total = rs_e(0)
        x2_new = x2[other] - total
        x2[slot] = x2_new
        n2[rows(me * seq), :] = rms(x2_new)[0].astype(BF16)
        ag_f(0)
        rs_c(1)
        ag_g(0)
        rs_d(1)
        ag_h(0)
        for cp in now[2:]:
            cp.wait()
        ag_i(0)
        out_copy(4, n2, n2_o, layer).start()
        qkv[...] = mm(n2[...], wqkv_s[...], NT).astype(BF16)
        key, val = qkv[:, qw:qw + hd], qkv[:, qw + hd:qw + 2 * hd]
        for r in range(heads):
            sc = mm(qkv[:, r * hd:(r + 1) * hd], key, NT) * scale
            sc = jnp.where(mask[...] > 0.5, sc, MASK_VALUE)
            ex = jnp.exp(sc - jnp.max(sc, axis=-1, keepdims=True))
            pr = ex / jnp.sum(ex, axis=-1, keepdims=True)
            probs[r] = pr
            att[:, r * hd:(r + 1) * hd] = mm(pr.astype(BF16), val, NN).astype(BF16)
        out_copy(5, att, a_o, layer).start()
        total = rs_e(1)
        norm, inv = rms(x1[other])
        dy1_new = dy1[...] + inv * (total - norm * jnp.mean(total * norm, axis=-1, keepdims=True))
        dy1[...] = dy1_new
        cc[rows(me * seq), :] = dy1_new.astype(BF16)
        ag_f(1)
        product(2, att, wo_s)
        out_copy(0, n1, n1_o, layer).wait()
        rs_a(2)
        rs_b(2)
        ag_g(1)
        rs_c(2)
        rs_d(2)
        ag_h(1)
        ag_i(1)
        out_copy(6, cc, c_o, layer).start()
        d_att = mm(cc[...], wo_s[...], NT).astype(BF16)
        d_key = jnp.zeros((tokens, hd), F32)
        d_val = jnp.zeros((tokens, hd), F32)
        for r in range(heads):
            da = d_att[:, r * hd:(r + 1) * hd]
            pr = probs[r]
            dp = mm(da, val, NT)
            ds = (pr * (dp - jnp.sum(dp * pr, axis=-1, keepdims=True)) * scale).astype(BF16)
            dqkv[:, r * hd:(r + 1) * hd] = mm(ds, key, NN).astype(BF16)
            d_key = d_key + mm(ds, qkv[:, r * hd:(r + 1) * hd], TN)
            d_val = d_val + mm(pr.astype(BF16), da, TN)
        dqkv[:, qw:qw + hd] = d_key.astype(BF16)
        dqkv[:, qw + hd:qw + 2 * hd] = d_val.astype(BF16)
        out_copy(7, dqkv, d_o, layer).start()
        product(3, dqkv, wqkv_s)
        out_copy(2, ee, e_o, layer).wait()
        rs_a(3)
        rs_b(3)

        @pl.when(end)
        def _():
            rs_c(3)
            fin_start(1, x2[slot])
        total = rs_e(2)
        x1_new = x1[other] - total
        x1[slot] = x1_new
        n1[rows(me * seq), :] = rms(x1_new)[0].astype(BF16)

        @pl.when(more)
        def _():
            ag_f(2)
            rs_c(3)
            ag_g(2)
            rs_d(3)
            ag_h(2)

        @pl.when(end)
        def _():
            rs_d(3)
            fin_start(2, dy1[...])
            fin_start(0, x1_new)
            ag_g(5)
            total = rs_e(3)
            norm, inv = rms(x2[slot])
            fin_start(3, dy2[...] + inv * (total - norm * jnp.mean(total * norm, axis=-1, keepdims=True)))
            ag_g(6)
            ag_h(5)
            ag_g(4)
            ag_h(6)
            fin_end(1)
            ag_h(4)
            fin_end(2)
        for k, src, dst in ((1, h_s, h_o), (3, u_s, u_o), (4, n2, n2_o), (5, att, a_o), (6, cc, c_o), (7, dqkv, d_o)):
            out_copy(k, src, dst, layer).wait()

    ag_g(7)
    ag_h(7)
    fin_end(0)
    fin_end(3)
    for k in range(4):
        fin_copy(k).wait()


def grad_kernel(parts, n1, n2, c_val, e_val, h_val, u_val, a_val, d_val, *refs):
    qw, hd = parts
    ends_in, (g_up, g_down, g_q, g_k, g_v, g_out), ends_out = refs[:4], refs[4:10], refs[10:]
    for src, dst in zip(ends_in, ends_out):
        dst[...] = src[...]
    g_up[0] = mm(u_val[0], n1[0], TN)
    g_down[0] = mm(h_val[0], e_val[0], TN)
    g_out[0] = mm(a_val[0], c_val[0], TN)
    g_all = mm(d_val[0], n2[0], TN)
    g_q[0] = g_all[:qw]
    g_k[0] = g_all[qw:qw + hd]
    g_v[0] = g_all[qw + hd:]


def solution(mesh):
    tp = mesh.shape['tp']
    assert tp == 8
    act_spec = P('dp', None, None)
    w_specs = (P(None, None, 'tp', None), P(None, None, 'tp', None), P(None, None, 'tp', None),
               P(None, 'tp', None, None), P(None, None, 'tp'), P(None, 'tp', None))
    g_specs = (P('dp', None, 'tp', None), P('dp', None, 'tp', None), P('dp', None, 'tp', None),
               P('dp', 'tp', None, None), P('dp', None, 'tp'), P('dp', 'tp', None))

    def local_fn(y_one, y_two, dy_one, dy_two, seq_lens, w_query, w_key, w_value, w_out, w_up, w_down):
        batch, seq, width = y_one.shape
        n_layers, _, heads, hd = w_query.shape
        assert batch == tp and w_key.shape[2] == 1
        tokens = batch * seq
        ff = w_down.shape[1]
        qw = heads * hd
        half = seq // 2
        acts = [x.reshape(tokens, width) for x in (y_one, y_two, dy_one, dy_two)]

        def flip(w):
            return w.transpose(0, 2, 3, 1).reshape(n_layers, -1, width)
        weights = (w_up.transpose(0, 2, 1), w_down, flip(w_query), flip(w_key), flip(w_value), w_out.reshape(n_layers, qw, width))

        def stack(cols):
            return jax.ShapeDtypeStruct((n_layers, tokens, cols), BF16)
        any_spec = pl.BlockSpec(memory_space=pl.ANY)
        vm = pltpu.VMEM
        dma = pltpu.SemaphoreType.DMA
        scratch = [vm((tokens, width), BF16)] * 4 + [
            vm((2, ff, width), BF16), vm((2, ff, width), BF16), vm((2, qw + 2 * hd, width), BF16), vm((2, qw, width), BF16),
            vm((tokens, ff), BF16), vm((tokens, ff), BF16), vm((tokens, ff), F32),
            vm((tokens, qw + 2 * hd), BF16), vm((tokens, qw), BF16), vm((tokens, qw + 2 * hd), BF16),
            vm((heads, tokens, tokens), F32), vm((tokens, tokens), F32),
            vm((2, seq, width), F32), vm((2, seq, width), F32), vm((seq, width), F32), vm((seq, width), F32),
            vm((4, tokens, width), F32), vm((4, 4, seq, width), F32), vm((4, 2, half, width), F32), vm((4, 2, seq, width), F32),
            vm((4, tokens, width), F32),
            dma((2, 6)), dma((6,)), dma((8,)), dma((4,)), dma((4, 10)), dma((4, 10)), dma((8, 9)), dma((8, 9))]
        *ends, n1, n2, c_val, e_val, h_val, u_val, a_val, d_val = pl.pallas_call(
            functools.partial(chain_kernel, (n_layers, tp, seq, width, heads, hd)),
            out_shape=(jax.ShapeDtypeStruct((tokens, width), F32),) * 4 + (stack(width), stack(width), stack(width), stack(width),
                       stack(ff), stack(ff), stack(qw), stack(qw + 2 * hd)),
            in_specs=[pl.BlockSpec(memory_space=pltpu.SMEM)] + [any_spec] * 10,
            out_specs=(any_spec,) * 12,
            scratch_shapes=scratch,
            compiler_params=pltpu.CompilerParams(collective_id=0, has_side_effects=True, vmem_limit_bytes=66_000_000),
            name='chain',
        )(seq_lens, *acts, *weights)

        col_tile = 512

        def wide():
            return pl.BlockSpec((1, tokens, col_tile), lambda layer, j: (layer, 0, j))

        def small(cols):
            return pl.BlockSpec((1, tokens, cols), lambda layer, j: (layer, 0, 0))
        g_rows = (ff, ff, qw, hd, hd, qw)
        moved = 2 * n_layers * tokens * (4 * width + 2 * ff + 2 * qw + 2 * hd) + 4 * n_layers * width * sum(g_rows)
        steps = n_layers * (width // col_tile)
        end_spec = pl.BlockSpec((tokens // steps, width), lambda layer, j: (layer * (width // col_tile) + j, 0))
        g_up, g_down, g_q, g_k, g_v, g_out, *ends = pl.pallas_call(
            functools.partial(grad_kernel, (qw, hd)),
            grid=(n_layers, width // col_tile),
            out_shape=tuple(jax.ShapeDtypeStruct((n_layers, r, width), F32) for r in g_rows) + (jax.ShapeDtypeStruct((tokens, width), F32),) * 4,
            in_specs=[wide()] * 4 + [small(ff), small(ff), small(qw), small(qw + 2 * hd)] + [end_spec] * 4,
            out_specs=tuple(pl.BlockSpec((1, r, col_tile), lambda layer, j: (layer, 0, j)) for r in g_rows) + (end_spec,) * 4,
            compiler_params=pltpu.CompilerParams(vmem_limit_bytes=60_000_000),
            cost_estimate=pl.CostEstimate(flops=2 * n_layers * tokens * width * sum(g_rows), bytes_accessed=moved, transcendentals=0),
            name='grads',
        )(n1, n2, c_val, e_val, h_val, u_val, a_val, d_val, *ends)

        def flip_back(g, like):
            return g.reshape(n_layers, -1, hd, width).transpose(0, 3, 1, 2).reshape(like.shape)
        dw_up, dw_down, dw_out = g_up.transpose(0, 2, 1), g_down, g_out.reshape(w_out.shape)
        dw_query, dw_key, dw_value = flip_back(g_q, w_query), flip_back(g_k, w_key), flip_back(g_v, w_value)
        ends = tuple(v.reshape(batch, seq, width) for v in ends)
        return ends + (dw_query, dw_key, dw_value, dw_out, dw_up, dw_down)

    return jax.shard_map(local_fn, mesh=mesh,
                         in_specs=(act_spec,) * 4 + (P('dp'),) + w_specs,
                         out_specs=(act_spec,) * 4 + g_specs,
                         check_vma=False)
```

```python
import functools

import jax
import jax.numpy as jnp
from jax import lax
from jax.experimental import pallas as pl
from jax.experimental.pallas import tpu as pltpu
from jax.sharding import PartitionSpec as P

F32 = jnp.float32
BF16 = jnp.bfloat16
EPS = 1e-5
MASK_VALUE = -1e30
GELU_C = 0.7978845608028654
GELU_A = 0.044715
MESH = pl.DeviceIdType.MESH
NT = (((1,), (1,)), ((), ()))
NN = (((1,), (0,)), ((), ()))
TN = (((0,), (0,)), ((), ()))


def mm(lhs, rhs, dims):
    return lax.dot_general(lhs, rhs, dims, preferred_element_type=F32)


def chain_kernel(cfg, lens, y1_h, y2_h, dy1_h, dy2_h, w1_h, w2_h, wq_h, wk_h, wv_h, wo_h,
                 f_x1, f_x2, f_dy1, f_dy2, n1_o, n2_o, c_o, e_o, h_o, u_o, a_o, d_o,
                 n1, n2, cc, ee, w1, w2, wqkv, wo, h_s, u_s, gp, qkv, att, dqkv, probs, mask,
                 x1, x2, dy1, dy2, part, ra, rb, rc, fbuf,
                 w_sem, in_sem, out_sem, fin_sem, rs_send, rs_recv, ag_send, ag_recv):
    n_layers, tp, seq, width, heads, hd = cfg
    chips = tp // 2
    tokens = tp * seq
    ht = tokens // 2
    own = ht // tp
    hw = width // 2
    scale = hd ** -0.5
    qw = heads * hd
    me = lax.axis_index('tp')
    chip = me // 2
    core = me - 2 * chip
    partner = me + 1 - 2 * core
    right = lax.rem(me + 2, tp)
    left = lax.rem(me + tp - 2, tp)
    opp = lax.rem(me + chips, tp)
    lo, hi, every = pl.ds(0, hw), pl.ds(hw, hw), pl.ds(0, width)
    halves = (pl.ds(0, ht), pl.ds(ht, ht))

    def rows(hb, who):
        return pl.ds(pl.multiple_of(hb * ht + who * own, own), own)

    def rcopy(src, dst, send, recv, dev):
        return pltpu.make_async_remote_copy(src_ref=src, dst_ref=dst, send_sem=send, recv_sem=recv,
                                            device_id={'tp': dev}, device_id_type=MESH)

    def w_copies(step):
        layer = n_layers - 1 - step
        slot = lax.rem(step, 2)
        kw = wk_h.shape[1]
        return (pltpu.make_async_copy(w1_h.at[layer], w1.at[slot], w_sem.at[slot, 0]),
                pltpu.make_async_copy(w2_h.at[layer], w2.at[slot], w_sem.at[slot, 1]),
                pltpu.make_async_copy(wq_h.at[layer], wqkv.at[slot, pl.ds(0, qw)], w_sem.at[slot, 2]),
                pltpu.make_async_copy(wk_h.at[layer], wqkv.at[slot, pl.ds(qw, kw)], w_sem.at[slot, 3]),
                pltpu.make_async_copy(wv_h.at[layer], wqkv.at[slot, pl.ds(qw + kw, kw)], w_sem.at[slot, 4]),
                pltpu.make_async_copy(wo_h.at[layer], wo.at[slot], w_sem.at[slot, 5]))

    owners = (opp, right, left, me)

    def rs_d2d(i, role):
        theirs = owners[role] + 1 - 2 * core
        return rcopy(part.at[i, rows(0, theirs)], ra.at[i, role], rs_send.at[i, role], rs_recv.at[i, role], partner)

    def rs_ring(i, kind):
        who, cols, dst, dev = ((opp, lo, rb.at[i, 0], right), (opp, hi, rb.at[i, 1], left),
                               (right, hi, rc.at[i, 0, :, hi], right), (left, lo, rc.at[i, 1, :, lo], left),
                               (right, lo, rc.at[i, 0, :, lo], right), (left, hi, rc.at[i, 1, :, hi], left))[kind]
        return rcopy(part.at[i, rows(0, who), cols], dst, rs_send.at[i, 4 + kind], rs_recv.at[i, 4 + kind], dev)

    def rs_add(i, who, cols, extra):
        r = rows(0, who)
        part[i, r, cols] = part[i, r, cols] + extra

    def rs_a(i):
        for role in range(4):
            rs_d2d(i, role).start()

    def rs_b(i):
        rs_d2d(i, 0).wait_recv()
        rs_add(i, opp, every, ra[i, 0])
        rs_ring(i, 0).start()
        rs_ring(i, 1).start()

    def rs_c(i):
        rs_d2d(i, 1).wait_recv()
        rs_add(i, right, every, ra[i, 1])
        rs_ring(i, 2).start()
        rs_d2d(i, 2).wait_recv()
        rs_add(i, left, every, ra[i, 2])
        rs_ring(i, 3).start()

    def rs_d(i):
        rs_ring(i, 0).wait_recv()
        rs_add(i, right, lo, rb[i, 0])
        rs_ring(i, 4).start()
        rs_ring(i, 1).wait_recv()
        rs_add(i, left, hi, rb[i, 1])
        rs_ring(i, 5).start()

    def rs_e(i):
        rs_d2d(i, 3).wait_recv()
        for kind in range(2, 6):
            rs_ring(i, kind).wait_recv()
        for role in range(4):
            rs_d2d(i, role).wait_send()
        for kind in range(6):
            rs_ring(i, kind).wait_send()
        return (part[i, rows(0, me), :] + ra[i, 3]) + (rc[i, 0] + rc[i, 1])

    bufs = (n2, n2, cc, cc, n1, n1, ee, ee)
    f_pos = (1, 1, 2, 2, 0, 0, 3, 3)
    f_out = (f_x1, f_x2, f_dy1, f_dy2)

    def ag_msg(i, kind, fin, receive=False):
        buf = fbuf.at[f_pos[i]] if fin else bufs[i]
        if receive:
            whos = (left, right, partner, opp, opp, lax.rem(partner + tp - 2, tp), lax.rem(partner + 2, tp),
                    lax.rem(partner + chips, tp), lax.rem(partner + chips, tp))
        else:
            whos = (me, me, me, left, right, left, right, opp, opp)
        cols = (every, every, every, lo, hi, every, every, lo, hi)[kind]
        dev = (right, left, partner, right, left, partner, partner, partner, partner)[kind]
        ref = buf.at[rows(i % 2, whos[kind]), cols]
        return rcopy(ref, ref, ag_send.at[i, kind], ag_recv.at[i, kind], dev)

    def ag_f(i, fin=False):
        for kind in range(3):
            ag_msg(i, kind, fin).start()

    def ag_g(i, fin=False):
        ag_msg(i, 0, fin, True).wait_recv()
        ag_msg(i, 3, fin).start()
        ag_msg(i, 5, fin).start()
        ag_msg(i, 1, fin, True).wait_recv()
        ag_msg(i, 4, fin).start()
        ag_msg(i, 6, fin).start()

    def ag_h(i, fin=False):
        ag_msg(i, 3, fin, True).wait_recv()
        ag_msg(i, 7, fin).start()
        ag_msg(i, 4, fin, True).wait_recv()
        ag_msg(i, 8, fin).start()

    def fin_copy(i):
        r = halves[i % 2]
        return pltpu.make_async_copy(fbuf.at[f_pos[i], r], f_out[f_pos[i]].at[r], fin_sem.at[i])

    def ag_i(i, fin=False):
        for kind in (2, 5, 6, 7, 8):
            ag_msg(i, kind, fin, True).wait_recv()
        for kind in range(9):
            ag_msg(i, kind, fin).wait_send()
        if fin:
            fin_copy(i).start()

    def fin_start(i, value):
        fbuf[f_pos[i], rows(i % 2, me), :] = value
        ag_f(i, True)

    def out_copy(k, hb, src, dst, layer):
        r = halves[hb]
        return pltpu.make_async_copy(src.at[r], dst.at[layer, r], out_sem.at[k, hb])

    def rms(x_val):
        inv = lax.rsqrt(jnp.mean(x_val * x_val, axis=-1, keepdims=True) + EPS)
        return x_val * inv, inv

    def rms_back(x_val, grad):
        norm, inv = rms(x_val)
        return inv * (grad - norm * jnp.mean(grad * norm, axis=-1, keepdims=True))

    barrier = pltpu.get_barrier_semaphore()
    for other in (partner, right, left):
        pl.semaphore_signal(barrier, inc=1, device_id={'tp': other}, device_id_type=MESH)
    y_loads = [pltpu.make_async_copy(y1_h.at[halves[hb]], part.at[4 + hb], in_sem.at[hb]) for hb in range(2)]
    d_loads = [pltpu.make_async_copy(dy2_h.at[halves[hb]], part.at[6 + hb], in_sem.at[2 + hb]) for hb in range(2)]
    loads = []
    for hb in range(2):
        r = rows(hb, me)
        for k, (src, dst) in enumerate(((y1_h, x1.at[1, hb]), (y2_h, x2.at[1, hb]), (dy1_h, dy1.at[hb]), (dy2_h, dy2.at[hb]))):
            loads.append(pltpu.make_async_copy(src.at[r], dst, in_sem.at[4 + 4 * hb + k]))
    first = w_copies(0)
    for cp in (y_loads[0], first[0], y_loads[1], first[1], *d_loads, *loads, *first[2:]):
        cp.start()
    chunk = 32
    for hb in range(2):
        y_loads[hb].wait()

        @pl.loop(0, ht // chunk)
        def _(b):
            src = pl.ds(pl.multiple_of(b * chunk, chunk), chunk)
            n1[pl.ds(pl.multiple_of(hb * ht + b * chunk, chunk), chunk), :] = rms(part[4 + hb, src, :])[0].astype(BF16)
    pl.semaphore_wait(barrier, 3)

    col_tile = 512

    def product(i, lhs_ref, w_ref):
        @pl.loop(0, width // col_tile)
        def _(j):
            cols = pl.ds(pl.multiple_of(j * col_tile, col_tile), col_tile)
            part[i, :, cols] = mm(lhs_ref[halves[i % 2], :], w_ref[:, cols], NN)

    def finish(i, slot, fin):
        hb = i % 2
        mine = rows(hb, me)
        total = rs_e(i)
        if i < 2:
            new = x2[1 - slot, hb] - total
            x2[slot, hb] = new
            n2[mine, :] = rms(new)[0].astype(BF16)
        elif i < 4:
            new = dy1[hb] + rms_back(x1[1 - slot, hb], total)
            dy1[hb] = new
            cc[mine, :] = new.astype(BF16)
        elif i < 6:
            new = x1[1 - slot, hb] - total
            x1[slot, hb] = new
            n1[mine, :] = rms(new)[0].astype(BF16)
        else:
            new = dy2[hb] + rms_back(x2[slot, hb], total)
            dy2[hb] = new
            ee[mine, :] = new.astype(BF16)
        if fin is True:
            fin_start(i, new)
        elif fin is False:
            ag_f(i)
        else:
            pl.when(fin)(lambda: fin_start(i, new))
            pl.when(jnp.logical_not(fin))(lambda: ag_f(i))

    def either(fn, i, end):
        if i < 4:
            fn(i)
        else:
            pl.when(end)(lambda: fn(i, True))
            pl.when(jnp.logical_not(end))(lambda: fn(i))

    @pl.loop(0, n_layers)
    def _(step):
        layer = n_layers - 1 - step
        slot = lax.rem(step, 2)
        w1_s, w2_s, wqkv_s, wo_s = w1.at[slot], w2.at[slot], wqkv.at[slot], wo.at[slot]
        later = step > 0
        more = step < n_layers - 1
        end = step == n_layers - 1
        now = w_copies(step)

        def compute(i):
            hb = i % 2
            r = halves[hb]
            if i == 0:
                now[0].wait()

                @pl.when(more)
                def _():
                    for cp in w_copies(step + 1):
                        cp.start()
            if i < 2:
                out_copy(0, hb, n1, n1_o, layer).start()
                pre = mm(n1[r, :], w1_s[...], NT)
                tan = jnp.tanh(GELU_C * (pre + GELU_A * (pre * pre * pre)))
                cdf = 0.5 * (1.0 + tan)
                h_s[r, :] = (pre * cdf).astype(BF16)
                gp[r, :] = cdf + pre * (0.5 * GELU_C) * (1.0 - tan * tan) * (1.0 + (3.0 * GELU_A) * (pre * pre))
                out_copy(1, hb, h_s, h_o, layer).start()
            elif i < 4:
                out_copy(2, hb, ee, e_o, layer).start()
                u_s[r, :] = (gp[r, :] * mm(ee[r, :], w2_s[...], NT)).astype(BF16)
                out_copy(3, hb, u_s, u_o, layer).start()
            elif i < 6:
                if i == 4:
                    for cp in now[2:]:
                        cp.wait()
                out_copy(4, hb, n2, n2_o, layer).start()
                qkv[r, :] = mm(n2[r, :], wqkv_s[...], NT).astype(BF16)
                key, val = qkv[r, qw:qw + hd], qkv[r, qw + hd:qw + 2 * hd]
                seen = mask[hb] > 0.5
                for head in range(heads):
                    cols = pl.ds(head * hd, hd)
                    sc = jnp.where(seen, mm(qkv[r, cols], key, NT) * scale, MASK_VALUE)
                    ex = jnp.exp(sc - jnp.max(sc, axis=-1, keepdims=True))
                    pr = ex / jnp.sum(ex, axis=-1, keepdims=True)
                    probs[head, r, :] = pr
                    att[r, cols] = mm(pr.astype(BF16), val, NN).astype(BF16)
                out_copy(5, hb, att, a_o, layer).start()
            else:
                out_copy(6, hb, cc, c_o, layer).start()
                d_att = mm(cc[r, :], wo_s[...], NT).astype(BF16)
                key, val = qkv[r, qw:qw + hd], qkv[r, qw + hd:qw + 2 * hd]
                d_key = jnp.zeros((ht, hd), F32)
                d_val = jnp.zeros((ht, hd), F32)
                for head in range(heads):
                    cols = pl.ds(head * hd, hd)
                    da = d_att[:, head * hd:(head + 1) * hd]
                    pr = probs[head, r, :]
                    dp = mm(da, val, NT)
                    ds = (pr * (dp - jnp.sum(dp * pr, axis=-1, keepdims=True)) * scale).astype(BF16)
                    dqkv[r, cols] = mm(ds, key, NN).astype(BF16)
                    d_key = d_key + mm(ds, qkv[r, cols], TN)
                    d_val = d_val + mm(pr.astype(BF16), da, TN)
                dqkv[r, qw:qw + hd] = d_key.astype(BF16)
                dqkv[r, qw + hd:qw + 2 * hd] = d_val.astype(BF16)
                out_copy(7, hb, dqkv, d_o, layer).start()

        def send(i):
            hb = i % 2
            if i == 0:
                now[1].wait()
            product(i, (h_s, u_s, att, dqkv)[i // 2], (w2_s, w1_s, wo_s, wqkv_s)[i // 2])
            if 4 <= i < 6:
                out_copy(0, hb, n1, n1_o, layer).wait()
            if i >= 6:
                out_copy(2, hb, ee, e_o, layer).wait()
            rs_a(i)

        def guarded(fn, i, back):
            w = (i - back) % 8
            if i < back:
                pl.when(later)(lambda: fn(w))
            elif fn is rs_d:
                fn(w)
            else:
                either(fn, w, end)

        for i in range(8):
            if i < 2:
                pl.when(later)(lambda: finish((i - 2) % 8, 1 - slot, False))
            else:
                finish(i - 2, slot, end if i >= 6 else False)
            compute(i)
            guarded(rs_d, i, 1)
            guarded(ag_h, i, 3)
            send(i)
            rs_b(i)
            guarded(ag_g, i, 2)
            rs_c(i)
            guarded(ag_i, i, 3)
            if i == 0:
                @pl.when(step == 0)
                def _():
                    for hb in range(2):
                        d_loads[hb].wait()

                        @pl.loop(0, ht // chunk)
                        def _(b):
                            src = pl.ds(pl.multiple_of(b * chunk, chunk), chunk)
                            ee[pl.ds(pl.multiple_of(hb * ht + b * chunk, chunk), chunk), :] = part[6 + hb, src, :].astype(BF16)
                        row_id = lax.broadcasted_iota(jnp.int32, (ht, ht), 0)
                        col_id = lax.broadcasted_iota(jnp.int32, (ht, ht), 1)
                        seen = jnp.zeros((ht, ht), F32)
                        for b in range(ht // seq):
                            inside = ((row_id < (b + 1) * seq) & (col_id >= b * seq) & (col_id <= row_id)
                                      & (col_id < b * seq + lens[hb * (ht // seq) + b]))
                            seen = jnp.where(inside, 1.0, seen)
                        mask[hb] = seen
                    for cp in loads:
                        cp.wait()
            if i == 6:
                @pl.when(end)
                def _():
                    fin_start(0, x2[slot, 0])
                    fin_start(1, x2[slot, 1])
            if i == 7:
                @pl.when(end)
                def _():
                    ag_g(0, True)
                    ag_g(1, True)
        for hb in range(2):
            for k, src, dst in ((1, h_s, h_o), (3, u_s, u_o), (4, n2, n2_o), (5, att, a_o), (6, cc, c_o), (7, dqkv, d_o)):
                out_copy(k, hb, src, dst, layer).wait()

    last = (n_layers - 1) % 2
    rs_d(7)
    finish(6, last, True)
    fin_start(2, dy1[0])
    ag_h(5, True)
    ag_h(0, True)
    ag_h(1, True)
    finish(7, last, True)
    fin_start(3, dy1[1])
    for i in (6, 2, 7, 3):
        ag_g(i, True)
    for i in (5, 0, 1):
        ag_i(i, True)
    for i in (6, 2, 7, 3):
        ag_h(i, True)
    for i in (6, 2, 7, 3):
        ag_i(i, True)
    for i in range(8):
        fin_copy(i).wait()


def grad_kernel(parts, n1, n2, c_val, e_val, h_val, u_val, a_val, d_val, *refs):
    qw, hd = parts
    ends_in, (g_up, g_down, g_q, g_k, g_v, g_out), ends_out = refs[:4], refs[4:10], refs[10:]
    for src, dst in zip(ends_in, ends_out):
        dst[...] = src[...]
    g_up[0] = mm(u_val[0], n1[0], TN)
    g_down[0] = mm(h_val[0], e_val[0], TN)
    g_out[0] = mm(a_val[0], c_val[0], TN)
    g_all = mm(d_val[0], n2[0], TN)
    g_q[0] = g_all[:qw]
    g_k[0] = g_all[qw:qw + hd]
    g_v[0] = g_all[qw + hd:]


def solution(mesh):
    tp = mesh.shape['tp']
    assert tp == 8
    act_spec = P('dp', None, None)
    w_specs = (P(None, None, 'tp', None), P(None, None, 'tp', None), P(None, None, 'tp', None),
               P(None, 'tp', None, None), P(None, None, 'tp'), P(None, 'tp', None))
    g_specs = (P('dp', None, 'tp', None), P('dp', None, 'tp', None), P('dp', None, 'tp', None),
               P('dp', 'tp', None, None), P('dp', None, 'tp'), P('dp', 'tp', None))

    def local_fn(y_one, y_two, dy_one, dy_two, seq_lens, w_query, w_key, w_value, w_out, w_up, w_down):
        batch, seq, width = y_one.shape
        n_layers, _, heads, hd = w_query.shape
        assert batch == tp and w_key.shape[2] == 1
        tokens = batch * seq
        ff = w_down.shape[1]
        qw = heads * hd
        ht = tokens // 2
        own = ht // tp
        assert ht % seq == 0 and own % 16 == 0
        acts = [x.reshape(tokens, width) for x in (y_one, y_two, dy_one, dy_two)]

        def flip(w):
            return w.transpose(0, 2, 3, 1).reshape(n_layers, -1, width)
        weights = (w_up.transpose(0, 2, 1), w_down, flip(w_query), flip(w_key), flip(w_value), w_out.reshape(n_layers, qw, width))

        def stack(cols):
            return jax.ShapeDtypeStruct((n_layers, tokens, cols), BF16)
        any_spec = pl.BlockSpec(memory_space=pl.ANY)
        vm = pltpu.VMEM
        dma = pltpu.SemaphoreType.DMA
        scratch = [vm((tokens, width), BF16)] * 4 + [
            vm((2, ff, width), BF16), vm((2, ff, width), BF16), vm((2, qw + 2 * hd, width), BF16), vm((2, qw, width), BF16),
            vm((tokens, ff), BF16), vm((tokens, ff), BF16), vm((tokens, ff), F32),
            vm((tokens, qw + 2 * hd), BF16), vm((tokens, qw), BF16), vm((tokens, qw + 2 * hd), BF16),
            vm((heads, tokens, ht), F32), vm((2, ht, ht), F32),
            vm((2, 2, own, width), F32), vm((2, 2, own, width), F32), vm((2, own, width), F32), vm((2, own, width), F32),
            vm((8, ht, width), F32), vm((8, 4, own, width), F32), vm((8, 2, own, width // 2), F32), vm((8, 2, own, width), F32),
            vm((4, tokens, width), F32),
            dma((2, 6)), dma((12,)), dma((8, 2)), dma((8,)), dma((8, 10)), dma((8, 10)), dma((8, 9)), dma((8, 9))]
        *ends, n1, n2, c_val, e_val, h_val, u_val, a_val, d_val = pl.pallas_call(
            functools.partial(chain_kernel, (n_layers, tp, seq, width, heads, hd)),
            out_shape=(jax.ShapeDtypeStruct((tokens, width), F32),) * 4 + (stack(width), stack(width), stack(width), stack(width),
                       stack(ff), stack(ff), stack(qw), stack(qw + 2 * hd)),
            in_specs=[pl.BlockSpec(memory_space=pltpu.SMEM)] + [any_spec] * 10,
            out_specs=(any_spec,) * 12,
            scratch_shapes=scratch,
            compiler_params=pltpu.CompilerParams(collective_id=0, has_side_effects=True, vmem_limit_bytes=66_000_000),
            name='chain',
        )(seq_lens, *acts, *weights)

        col_tile = 512

        def wide():
            return pl.BlockSpec((1, tokens, col_tile), lambda layer, j: (layer, 0, j))

        def small(cols):
            return pl.BlockSpec((1, tokens, cols), lambda layer, j: (layer, 0, 0))
        g_rows = (ff, ff, qw, hd, hd, qw)
        moved = 2 * n_layers * tokens * (4 * width + 2 * ff + 2 * qw + 2 * hd) + 4 * n_layers * width * sum(g_rows)
        steps = n_layers * (width // col_tile)
        end_spec = pl.BlockSpec((tokens // steps, width), lambda layer, j: (layer * (width // col_tile) + j, 0))
        g_up, g_down, g_q, g_k, g_v, g_out, *ends = pl.pallas_call(
            functools.partial(grad_kernel, (qw, hd)),
            grid=(n_layers, width // col_tile),
            out_shape=tuple(jax.ShapeDtypeStruct((n_layers, r, width), F32) for r in g_rows) + (jax.ShapeDtypeStruct((tokens, width), F32),) * 4,
            in_specs=[wide()] * 4 + [small(ff), small(ff), small(qw), small(qw + 2 * hd)] + [end_spec] * 4,
            out_specs=tuple(pl.BlockSpec((1, r, col_tile), lambda layer, j: (layer, 0, j)) for r in g_rows) + (end_spec,) * 4,
            compiler_params=pltpu.CompilerParams(vmem_limit_bytes=60_000_000),
            cost_estimate=pl.CostEstimate(flops=2 * n_layers * tokens * width * sum(g_rows), bytes_accessed=moved, transcendentals=0),
            name='grads',
        )(n1, n2, c_val, e_val, h_val, u_val, a_val, d_val, *ends)

        def flip_back(g, like):
            return g.reshape(n_layers, -1, hd, width).transpose(0, 3, 1, 2).reshape(like.shape)
        dw_up, dw_down, dw_out = g_up.transpose(0, 2, 1), g_down, g_out.reshape(w_out.shape)
        dw_query, dw_key, dw_value = flip_back(g_q, w_query), flip_back(g_k, w_key), flip_back(g_v, w_value)
        ends = tuple(v.reshape(batch, seq, width) for v in ends)
        return ends + (dw_query, dw_key, dw_value, dw_out, dw_up, dw_down)

    return jax.shard_map(local_fn, mesh=mesh,
                         in_specs=(act_spec,) * 4 + (P('dp'),) + w_specs,
                         out_specs=(act_spec,) * 4 + g_specs,
                         check_vma=False)
```

```python
import functools

import jax
import jax.numpy as jnp
from jax import lax
from jax.experimental import pallas as pl
from jax.experimental.pallas import tpu as pltpu
from jax.sharding import PartitionSpec as P

F32 = jnp.float32
BF16 = jnp.bfloat16
EPS = 1e-5
MASK_VALUE = -1e30
GELU_C = 0.7978845608028654
GELU_A = 0.044715
MESH = pl.DeviceIdType.MESH
NT = (((1,), (1,)), ((), ()))
NN = (((1,), (0,)), ((), ()))
TN = (((0,), (0,)), ((), ()))


def mm(lhs, rhs, dims):
    return lax.dot_general(lhs, rhs, dims, preferred_element_type=F32)


def chain_kernel(cfg, lens, y1_h, y2_h, dy1_h, dy2_h, w1_h, w2_h, wq_h, wk_h, wv_h, wo_h,
                 f_x1, f_x2, f_dy1, f_dy2, n1_o, n2_o, c_o, e_o, h_o, u_o, a_o, d_o,
                 n1, n2, cc, ee, w1, w2, wqkv, wo, h_s, u_s, gp, qkv, att, dqkv, probs, mask,
                 x1, x2, dy1, dy2, part, ra, rb, rc, fbuf,
                 w_sem, in_sem, out_sem, fin_sem, rs_send, rs_recv, ag_send, ag_recv):
    n_layers, tp, seq, width, heads, hd = cfg
    chips = tp // 2
    tokens = tp * seq
    ht = tokens // 2
    own = ht // tp
    hw = width // 2
    chunk = 32
    scale = hd ** -0.5
    qw = heads * hd
    me = lax.axis_index('tp')
    chip = me // 2
    core = me - 2 * chip
    partner = me + 1 - 2 * core
    right = lax.rem(me + 2, tp)
    left = lax.rem(me + tp - 2, tp)
    opp = lax.rem(me + chips, tp)
    lo, hi, every = pl.ds(0, hw), pl.ds(hw, hw), pl.ds(0, width)
    halves = (pl.ds(0, ht), pl.ds(ht, ht))

    def rows(hb, who):
        return pl.ds(pl.multiple_of(hb * ht + who * own, own), own)

    def rcopy(src, dst, send, recv, dev):
        return pltpu.make_async_remote_copy(src_ref=src, dst_ref=dst, send_sem=send, recv_sem=recv,
                                            device_id={'tp': dev}, device_id_type=MESH)

    def w_copies(step):
        layer = n_layers - 1 - step
        slot = lax.rem(step, 2)
        kw = wk_h.shape[1]
        return (pltpu.make_async_copy(w1_h.at[layer], w1.at[slot], w_sem.at[slot, 0]),
                pltpu.make_async_copy(w2_h.at[layer], w2.at[slot], w_sem.at[slot, 1]),
                pltpu.make_async_copy(wq_h.at[layer], wqkv.at[slot, pl.ds(0, qw)], w_sem.at[slot, 2]),
                pltpu.make_async_copy(wk_h.at[layer], wqkv.at[slot, pl.ds(qw, kw)], w_sem.at[slot, 3]),
                pltpu.make_async_copy(wv_h.at[layer], wqkv.at[slot, pl.ds(qw + kw, kw)], w_sem.at[slot, 4]),
                pltpu.make_async_copy(wo_h.at[layer], wo.at[slot], w_sem.at[slot, 5]))

    owners = (opp, right, left, me)

    def rs_d2d(i, role):
        theirs = owners[role] + 1 - 2 * core
        return rcopy(part.at[i, rows(0, theirs)], ra.at[i, role], rs_send.at[i, role], rs_recv.at[i, role], partner)

    def rs_ring(i, kind):
        who, cols, dst, dev = ((opp, lo, rb.at[i, 0], right), (opp, hi, rb.at[i, 1], left),
                               (right, hi, rc.at[i, 0, :, hi], right), (left, lo, rc.at[i, 1, :, lo], left),
                               (right, lo, rc.at[i, 0, :, lo], right), (left, hi, rc.at[i, 1, :, hi], left))[kind]
        return rcopy(part.at[i, rows(0, who), cols], dst, rs_send.at[i, 4 + kind], rs_recv.at[i, 4 + kind], dev)

    def rs_add(i, who, cols, extra):
        r = rows(0, who)
        part[i, r, cols] = part[i, r, cols] + extra

    def rs_a(i):
        for role in range(4):
            rs_d2d(i, role).start()

    def rs_b(i):
        rs_d2d(i, 0).wait_recv()
        rs_add(i, opp, every, ra[i, 0])
        rs_ring(i, 0).start()
        rs_ring(i, 1).start()

    def rs_c(i):
        rs_d2d(i, 1).wait_recv()
        rs_add(i, right, every, ra[i, 1])
        rs_ring(i, 2).start()
        rs_d2d(i, 2).wait_recv()
        rs_add(i, left, every, ra[i, 2])
        rs_ring(i, 3).start()

    def rs_d(i):
        rs_ring(i, 0).wait_recv()
        rs_add(i, right, lo, rb[i, 0])
        rs_ring(i, 4).start()
        rs_ring(i, 1).wait_recv()
        rs_add(i, left, hi, rb[i, 1])
        rs_ring(i, 5).start()

    def rs_e(i):
        rs_d2d(i, 3).wait_recv()
        for kind in range(2, 6):
            rs_ring(i, kind).wait_recv()
        for role in range(4):
            rs_d2d(i, role).wait_send()
        for kind in range(6):
            rs_ring(i, kind).wait_send()
        return (part[i, rows(0, me), :] + ra[i, 3]) + (rc[i, 0] + rc[i, 1])

    bufs = (n2, n2, cc, cc, n1, n1, ee, ee)
    f_pos = (1, 1, 2, 2, 0, 0, 3, 3)
    f_out = (f_x1, f_x2, f_dy1, f_dy2)

    def ag_msg(i, kind, fin, receive=False):
        buf = fbuf.at[f_pos[i]] if fin else bufs[i]
        if receive:
            whos = (left, right, partner, opp, opp, lax.rem(partner + tp - 2, tp), lax.rem(partner + 2, tp),
                    lax.rem(partner + chips, tp), lax.rem(partner + chips, tp))
        else:
            whos = (me, me, me, left, right, left, right, opp, opp)
        cols = (every, every, every, lo, hi, every, every, lo, hi)[kind]
        dev = (right, left, partner, right, left, partner, partner, partner, partner)[kind]
        ref = buf.at[rows(i % 2, whos[kind]), cols]
        return rcopy(ref, ref, ag_send.at[i, kind], ag_recv.at[i, kind], dev)

    def ag_f(i, fin=False):
        for kind in range(3):
            ag_msg(i, kind, fin).start()

    def ag_g(i, fin=False):
        ag_msg(i, 0, fin, True).wait_recv()
        ag_msg(i, 3, fin).start()
        ag_msg(i, 5, fin).start()
        ag_msg(i, 1, fin, True).wait_recv()
        ag_msg(i, 4, fin).start()
        ag_msg(i, 6, fin).start()

    def ag_h(i, fin=False):
        ag_msg(i, 3, fin, True).wait_recv()
        ag_msg(i, 7, fin).start()
        ag_msg(i, 4, fin, True).wait_recv()
        ag_msg(i, 8, fin).start()

    def fin_copy(i):
        r = halves[i % 2]
        return pltpu.make_async_copy(fbuf.at[f_pos[i], r], f_out[f_pos[i]].at[r], fin_sem.at[i])

    def ag_i(i, fin=False):
        for kind in (2, 5, 6, 7, 8):
            ag_msg(i, kind, fin, True).wait_recv()
        for kind in range(9):
            ag_msg(i, kind, fin).wait_send()
        if fin:
            fin_copy(i).start()
        if fin and i < 4:
            @pl.loop(0, ht // chunk)
            def _(b):
                r = pl.ds(pl.multiple_of((i % 2) * ht + b * chunk, chunk), chunk)
                got = fbuf[f_pos[i], r, :]
                bufs[i][r, :] = (rms(got)[0] if i < 2 else got).astype(BF16)

    def fin_start(i, value):
        fbuf[f_pos[i], rows(i % 2, me), :] = value
        ag_f(i, True)

    def out_copy(k, hb, src, dst, layer):
        r = halves[hb]
        return pltpu.make_async_copy(src.at[r], dst.at[layer, r], out_sem.at[k, hb])

    def rms(x_val):
        inv = lax.rsqrt(jnp.mean(x_val * x_val, axis=-1, keepdims=True) + EPS)
        return x_val * inv, inv

    def rms_back(x_val, grad):
        norm, inv = rms(x_val)
        return inv * (grad - norm * jnp.mean(grad * norm, axis=-1, keepdims=True))

    barrier = pltpu.get_barrier_semaphore()
    for other in (partner, right, left):
        pl.semaphore_signal(barrier, inc=1, device_id={'tp': other}, device_id_type=MESH)
    y_loads = [pltpu.make_async_copy(y1_h.at[halves[hb]], part.at[4 + hb], in_sem.at[hb]) for hb in range(2)]
    d_loads = [pltpu.make_async_copy(dy2_h.at[halves[hb]], part.at[6 + hb], in_sem.at[2 + hb]) for hb in range(2)]
    loads = []
    for hb in range(2):
        r = rows(hb, me)
        for k, (src, dst) in enumerate(((y1_h, x1.at[1, hb]), (y2_h, x2.at[1, hb]), (dy1_h, dy1.at[hb]), (dy2_h, dy2.at[hb]))):
            loads.append(pltpu.make_async_copy(src.at[r], dst, in_sem.at[4 + 4 * hb + k]))
    first = w_copies(0)
    y_loads[0].start()
    first[0].start()
    y_loads[0].wait()
    for cp in (first[1], y_loads[1], *d_loads, *loads, *first[2:]):
        cp.start()

    def rounded(dst, i, fn):
        @pl.loop(0, ht // chunk)
        def _(b):
            src = pl.ds(pl.multiple_of(b * chunk, chunk), chunk)
            dst[pl.ds(pl.multiple_of((i % 2) * ht + b * chunk, chunk), chunk), :] = fn(part[i, src, :]).astype(BF16)
    rounded(n1, 4, lambda x: rms(x)[0])
    pl.semaphore_wait(barrier, 3)

    col_tile = 512

    def product(i, lhs_ref, w_ref):
        @pl.loop(0, width // col_tile)
        def _(j):
            cols = pl.ds(pl.multiple_of(j * col_tile, col_tile), col_tile)
            part[i, :, cols] = mm(lhs_ref[halves[i % 2], :], w_ref[:, cols], NN)

    def finish(i, slot, fin):
        hb = i % 2
        mine = rows(hb, me)
        total = rs_e(i)
        if i < 2:
            new = x2[1 - slot, hb] - total
            x2[slot, hb] = new
        elif i < 4:
            new = dy1[hb] + rms_back(x1[1 - slot, hb], total)
            dy1[hb] = new
        elif i < 6:
            new = x1[1 - slot, hb] - total
            x1[slot, hb] = new
        else:
            new = dy2[hb] + rms_back(x2[slot, hb], total)
            dy2[hb] = new

        def send_b():
            bufs[i][mine, :] = (rms(new)[0] if i in (0, 1, 4, 5) else new).astype(BF16)
            ag_f(i)
        if fin is True:
            fin_start(i, new)
        elif fin is False:
            send_b()
        else:
            pl.when(fin)(lambda: fin_start(i, new))
            pl.when(jnp.logical_not(fin))(send_b)

    def either(fn, i, end):
        pl.when(end)(lambda: fn(i, True))
        pl.when(jnp.logical_not(end))(lambda: fn(i))

    @pl.loop(0, n_layers)
    def _(step):
        layer = n_layers - 1 - step
        slot = lax.rem(step, 2)
        w1_s, w2_s, wqkv_s, wo_s = w1.at[slot], w2.at[slot], wqkv.at[slot], wo.at[slot]
        later = step > 0
        more = step < n_layers - 1
        end = step == n_layers - 1
        now = w_copies(step)

        def compute(i):
            hb = i % 2
            r = halves[hb]
            if i == 0:
                now[0].wait()

                @pl.when(more)
                def _():
                    for cp in w_copies(step + 1):
                        cp.start()
            if i < 2:
                out_copy(0, hb, n1, n1_o, layer).start()
                pre = mm(n1[r, :], w1_s[...], NT)
                tan = jnp.tanh(GELU_C * (pre + GELU_A * (pre * pre * pre)))
                cdf = 0.5 * (1.0 + tan)
                h_s[r, :] = (pre * cdf).astype(BF16)
                gp[r, :] = cdf + pre * (0.5 * GELU_C) * (1.0 - tan * tan) * (1.0 + (3.0 * GELU_A) * (pre * pre))
                out_copy(1, hb, h_s, h_o, layer).start()
            elif i < 4:
                out_copy(2, hb, ee, e_o, layer).start()
                u_s[r, :] = (gp[r, :] * mm(ee[r, :], w2_s[...], NT)).astype(BF16)
                out_copy(3, hb, u_s, u_o, layer).start()
            elif i < 6:
                if i == 4:
                    for cp in now[2:]:
                        cp.wait()
                out_copy(4, hb, n2, n2_o, layer).start()
                qkv[r, :] = mm(n2[r, :], wqkv_s[...], NT).astype(BF16)
                key, val = qkv[r, qw:qw + hd], qkv[r, qw + hd:qw + 2 * hd]
                seen = mask[hb] > 0.5
                for head in range(heads):
                    cols = pl.ds(head * hd, hd)
                    sc = jnp.where(seen, mm(qkv[r, cols], key, NT) * scale, MASK_VALUE)
                    ex = jnp.exp(sc - jnp.max(sc, axis=-1, keepdims=True))
                    pr = ex / jnp.sum(ex, axis=-1, keepdims=True)
                    probs[head, r, :] = pr
                    att[r, cols] = mm(pr.astype(BF16), val, NN).astype(BF16)
                out_copy(5, hb, att, a_o, layer).start()
            else:
                out_copy(6, hb, cc, c_o, layer).start()
                d_att = mm(cc[r, :], wo_s[...], NT).astype(BF16)
                key, val = qkv[r, qw:qw + hd], qkv[r, qw + hd:qw + 2 * hd]
                d_key = jnp.zeros((ht, hd), F32)
                d_val = jnp.zeros((ht, hd), F32)
                for head in range(heads):
                    cols = pl.ds(head * hd, hd)
                    da = d_att[:, head * hd:(head + 1) * hd]
                    pr = probs[head, r, :]
                    dp = mm(da, val, NT)
                    ds = (pr * (dp - jnp.sum(dp * pr, axis=-1, keepdims=True)) * scale).astype(BF16)
                    dqkv[r, cols] = mm(ds, key, NN).astype(BF16)
                    d_key = d_key + mm(ds, qkv[r, cols], TN)
                    d_val = d_val + mm(pr.astype(BF16), da, TN)
                dqkv[r, qw:qw + hd] = d_key.astype(BF16)
                dqkv[r, qw + hd:qw + 2 * hd] = d_val.astype(BF16)
                out_copy(7, hb, dqkv, d_o, layer).start()

        def send(i):
            hb = i % 2
            if i == 0:
                now[1].wait()
            product(i, (h_s, u_s, att, dqkv)[i // 2], (w2_s, w1_s, wo_s, wqkv_s)[i // 2])
            if 4 <= i < 6:
                out_copy(0, hb, n1, n1_o, layer).wait()
            if i >= 6:
                out_copy(2, hb, ee, e_o, layer).wait()
            rs_a(i)

        def guarded(fn, i, back):
            w = (i - back) % 8
            if i < back:
                pl.when(later)(lambda: fn(w))
            elif fn is rs_d:
                fn(w)
            else:
                either(fn, w, end)

        for i in range(8):
            if i < 2:
                pl.when(later)(lambda: finish((i - 2) % 8, 1 - slot, False))
            else:
                finish(i - 2, slot, end)
            compute(i)
            guarded(rs_d, i, 1)
            guarded(ag_h, i, 3)
            send(i)
            if i == 0:
                @pl.when(step == 0)
                def _():
                    y_loads[1].wait()
                    rounded(n1, 5, lambda x: rms(x)[0])
            rs_b(i)
            guarded(ag_g, i, 2)
            rs_c(i)
            guarded(ag_i, i, 3)
            if i == 1:
                @pl.when(step == 0)
                def _():
                    for hb in range(2):
                        d_loads[hb].wait()
                        rounded(ee, 6 + hb, lambda x: x)
                        row_id = lax.broadcasted_iota(jnp.int32, (ht, ht), 0)
                        col_id = lax.broadcasted_iota(jnp.int32, (ht, ht), 1)
                        seen = jnp.zeros((ht, ht), F32)
                        for b in range(ht // seq):
                            inside = ((row_id < (b + 1) * seq) & (col_id >= b * seq) & (col_id <= row_id)
                                      & (col_id < b * seq + lens[hb * (ht // seq) + b]))
                            seen = jnp.where(inside, 1.0, seen)
                        mask[hb] = seen
                    for cp in loads:
                        cp.wait()
        for hb in range(2):
            for k, src, dst in ((1, h_s, h_o), (3, u_s, u_o), (4, n2, n2_o), (5, att, a_o), (6, cc, c_o), (7, dqkv, d_o)):
                out_copy(k, hb, src, dst, layer).wait()

    last = (n_layers - 1) % 2
    rs_d(7)
    finish(6, last, True)
    ag_h(5, True)
    finish(7, last, True)
    ag_i(5, True)
    for i in (6, 7):
        ag_g(i, True)
    for i in (6, 7):
        ag_h(i, True)
    for i in (6, 7):
        ag_i(i, True)
    for i in range(8):
        fin_copy(i).wait()


def grad_kernel(parts, n1, n2, c_val, e_val, h_val, u_val, a_val, d_val, *refs):
    qw, hd = parts
    ends_in, (g_up, g_down, g_q, g_k, g_v, g_out), ends_out = refs[:4], refs[4:10], refs[10:]
    for src, dst in zip(ends_in, ends_out):
        dst[...] = src[...]
    g_up[0] = mm(u_val[0], n1[0], TN)
    g_down[0] = mm(h_val[0], e_val[0], TN)
    g_out[0] = mm(a_val[0], c_val[0], TN)
    g_all = mm(d_val[0], n2[0], TN)
    g_q[0] = g_all[:qw]
    g_k[0] = g_all[qw:qw + hd]
    g_v[0] = g_all[qw + hd:]


def solution(mesh):
    tp = mesh.shape['tp']
    assert tp == 8
    act_spec = P('dp', None, None)
    w_specs = (P(None, None, 'tp', None), P(None, None, 'tp', None), P(None, None, 'tp', None),
               P(None, 'tp', None, None), P(None, None, 'tp'), P(None, 'tp', None))
    g_specs = (P('dp', None, 'tp', None), P('dp', None, 'tp', None), P('dp', None, 'tp', None),
               P('dp', 'tp', None, None), P('dp', None, 'tp'), P('dp', 'tp', None))

    def local_fn(y_one, y_two, dy_one, dy_two, seq_lens, w_query, w_key, w_value, w_out, w_up, w_down):
        batch, seq, width = y_one.shape
        n_layers, _, heads, hd = w_query.shape
        assert batch == tp and w_key.shape[2] == 1
        tokens = batch * seq
        ff = w_down.shape[1]
        qw = heads * hd
        ht = tokens // 2
        own = ht // tp
        assert ht % seq == 0 and own % 16 == 0
        acts = [x.reshape(tokens, width) for x in (y_one, y_two, dy_one, dy_two)]

        def flip(w):
            return w.transpose(0, 2, 3, 1).reshape(n_layers, -1, width)
        weights = (w_up.transpose(0, 2, 1), w_down, flip(w_query), flip(w_key), flip(w_value), w_out.reshape(n_layers, qw, width))

        def stack(cols):
            return jax.ShapeDtypeStruct((n_layers, tokens, cols), BF16)
        any_spec = pl.BlockSpec(memory_space=pl.ANY)
        vm = pltpu.VMEM
        dma = pltpu.SemaphoreType.DMA
        scratch = [vm((tokens, width), BF16)] * 4 + [
            vm((2, ff, width), BF16), vm((2, ff, width), BF16), vm((2, qw + 2 * hd, width), BF16), vm((2, qw, width), BF16),
            vm((tokens, ff), BF16), vm((tokens, ff), BF16), vm((tokens, ff), F32),
            vm((tokens, qw + 2 * hd), BF16), vm((tokens, qw), BF16), vm((tokens, qw + 2 * hd), BF16),
            vm((heads, tokens, ht), F32), vm((2, ht, ht), F32),
            vm((2, 2, own, width), F32), vm((2, 2, own, width), F32), vm((2, own, width), F32), vm((2, own, width), F32),
            vm((8, ht, width), F32), vm((8, 4, own, width), F32), vm((8, 2, own, width // 2), F32), vm((8, 2, own, width), F32),
            vm((4, tokens, width), F32),
            dma((2, 6)), dma((12,)), dma((8, 2)), dma((8,)), dma((8, 10)), dma((8, 10)), dma((8, 9)), dma((8, 9))]
        *ends, n1, n2, c_val, e_val, h_val, u_val, a_val, d_val = pl.pallas_call(
            functools.partial(chain_kernel, (n_layers, tp, seq, width, heads, hd)),
            out_shape=(jax.ShapeDtypeStruct((tokens, width), F32),) * 4 + (stack(width), stack(width), stack(width), stack(width),
                       stack(ff), stack(ff), stack(qw), stack(qw + 2 * hd)),
            in_specs=[pl.BlockSpec(memory_space=pltpu.SMEM)] + [any_spec] * 10,
            out_specs=(any_spec,) * 12,
            scratch_shapes=scratch,
            compiler_params=pltpu.CompilerParams(collective_id=0, has_side_effects=True, vmem_limit_bytes=66_000_000),
            name='chain',
        )(seq_lens, *acts, *weights)

        col_tile = 512

        def wide():
            return pl.BlockSpec((1, tokens, col_tile), lambda layer, j: (layer, 0, j))

        def small(cols):
            return pl.BlockSpec((1, tokens, cols), lambda layer, j: (layer, 0, 0))
        g_rows = (ff, ff, qw, hd, hd, qw)
        moved = 2 * n_layers * tokens * (4 * width + 2 * ff + 2 * qw + 2 * hd) + 4 * n_layers * width * sum(g_rows)
        steps = n_layers * (width // col_tile)
        end_spec = pl.BlockSpec((tokens // steps, width), lambda layer, j: (layer * (width // col_tile) + j, 0))
        g_up, g_down, g_q, g_k, g_v, g_out, *ends = pl.pallas_call(
            functools.partial(grad_kernel, (qw, hd)),
            grid=(n_layers, width // col_tile),
            out_shape=tuple(jax.ShapeDtypeStruct((n_layers, r, width), F32) for r in g_rows) + (jax.ShapeDtypeStruct((tokens, width), F32),) * 4,
            in_specs=[wide()] * 4 + [small(ff), small(ff), small(qw), small(qw + 2 * hd)] + [end_spec] * 4,
            out_specs=tuple(pl.BlockSpec((1, r, col_tile), lambda layer, j: (layer, 0, j)) for r in g_rows) + (end_spec,) * 4,
            compiler_params=pltpu.CompilerParams(vmem_limit_bytes=60_000_000),
            cost_estimate=pl.CostEstimate(flops=2 * n_layers * tokens * width * sum(g_rows), bytes_accessed=moved, transcendentals=0),
            name='grads',
        )(n1, n2, c_val, e_val, h_val, u_val, a_val, d_val, *ends)

        def flip_back(g, like):
            return g.reshape(n_layers, -1, hd, width).transpose(0, 3, 1, 2).reshape(like.shape)
        dw_up, dw_down, dw_out = g_up.transpose(0, 2, 1), g_down, g_out.reshape(w_out.shape)
        dw_query, dw_key, dw_value = flip_back(g_q, w_query), flip_back(g_k, w_key), flip_back(g_v, w_value)
        ends = tuple(v.reshape(batch, seq, width) for v in ends)
        return ends + (dw_query, dw_key, dw_value, dw_out, dw_up, dw_down)

    return jax.shard_map(local_fn, mesh=mesh,
                         in_specs=(act_spec,) * 4 + (P('dp'),) + w_specs,
                         out_specs=(act_spec,) * 4 + g_specs,
                         check_vma=False)
```

```python
import functools

import jax
import jax.numpy as jnp
from jax import lax
from jax.experimental import pallas as pl
from jax.experimental.pallas import tpu as pltpu
from jax.sharding import PartitionSpec as P

F32 = jnp.float32
BF16 = jnp.bfloat16
EPS = 1e-5
MASK_VALUE = -1e30
GELU_C = 0.7978845608028654
GELU_A = 0.044715
MESH = pl.DeviceIdType.MESH
NT = (((1,), (1,)), ((), ()))
NN = (((1,), (0,)), ((), ()))
TN = (((0,), (0,)), ((), ()))


def mm(lhs, rhs, dims):
    return lax.dot_general(lhs, rhs, dims, preferred_element_type=F32)


def chain_kernel(cfg, lens, y1_h, y2_h, dy1_h, dy2_h, w1_h, w2_h, wq_h, wk_h, wv_h, wo_h,
                 f_x1, f_x2, f_dy1, f_dy2, n1_o, n2_o, c_o, e_o, h_o, u_o, a_o, d_o,
                 n1, n2, cc, ee, w1, w2, wqkv, wo, h_s, u_s, gp, qkv, att, dqkv, probs, mask,
                 x1, x2, dy1, dy2, part, ra, rb, rc, fbuf,
                 w_sem, in_sem, out_sem, fin_sem, rs_send, rs_recv, ag_send, ag_recv):
    n_layers, tp, seq, width, heads, hd = cfg
    chips = tp // 2
    tokens = tp * seq
    ht = tokens // 2
    own = ht // tp
    hw = width // 2
    chunk = 32
    scale = hd ** -0.5
    qw = heads * hd
    me = lax.axis_index('tp')
    chip = me // 2
    core = me - 2 * chip
    partner = me + 1 - 2 * core
    right = lax.rem(me + 2, tp)
    left = lax.rem(me + tp - 2, tp)
    opp = lax.rem(me + chips, tp)
    lo, hi, every = pl.ds(0, hw), pl.ds(hw, hw), pl.ds(0, width)
    halves = (pl.ds(0, ht), pl.ds(ht, ht))

    def rows(hb, who):
        return pl.ds(pl.multiple_of(hb * ht + who * own, own), own)

    def rcopy(src, dst, send, recv, dev):
        return pltpu.make_async_remote_copy(src_ref=src, dst_ref=dst, send_sem=send, recv_sem=recv,
                                            device_id={'tp': dev}, device_id_type=MESH)

    def w_copies(step):
        layer = n_layers - 1 - step
        slot = lax.rem(step, 2)
        kw = wk_h.shape[1]
        return (pltpu.make_async_copy(w1_h.at[layer], w1.at[slot], w_sem.at[slot, 0]),
                pltpu.make_async_copy(w2_h.at[layer], w2.at[slot], w_sem.at[slot, 1]),
                pltpu.make_async_copy(wq_h.at[layer], wqkv.at[slot, pl.ds(0, qw)], w_sem.at[slot, 2]),
                pltpu.make_async_copy(wk_h.at[layer], wqkv.at[slot, pl.ds(qw, kw)], w_sem.at[slot, 3]),
                pltpu.make_async_copy(wv_h.at[layer], wqkv.at[slot, pl.ds(qw + kw, kw)], w_sem.at[slot, 4]),
                pltpu.make_async_copy(wo_h.at[layer], wo.at[slot], w_sem.at[slot, 5]))

    owners = (opp, right, left, me)

    def rs_d2d(i, role):
        theirs = owners[role] + 1 - 2 * core
        return rcopy(part.at[i, rows(0, theirs)], ra.at[i, role], rs_send.at[i, role], rs_recv.at[i, role], partner)

    def rs_ring(i, kind):
        who, cols, dst, dev = ((opp, lo, rb.at[i, 0], right), (opp, hi, rb.at[i, 1], left),
                               (right, hi, rc.at[i, 0, :, hi], right), (left, lo, rc.at[i, 1, :, lo], left),
                               (right, lo, rc.at[i, 0, :, lo], right), (left, hi, rc.at[i, 1, :, hi], left))[kind]
        return rcopy(part.at[i, rows(0, who), cols], dst, rs_send.at[i, 4 + kind], rs_recv.at[i, 4 + kind], dev)

    def rs_add(i, who, cols, extra):
        r = rows(0, who)
        part[i, r, cols] = part[i, r, cols] + extra

    n_tiles = 4
    tiles = [pl.ds(t * (width // n_tiles), width // n_tiles) for t in range(n_tiles)]

    def rs_first(i, t):
        theirs = opp + 1 - 2 * core
        pos = 10 + t
        return rcopy(part.at[i, rows(0, theirs), tiles[t]], ra.at[i, 0, :, tiles[t]], rs_send.at[i, pos], rs_recv.at[i, pos], partner)

    def rs_a(i):
        for role in range(1, 4):
            rs_d2d(i, role).start()

    def rs_b(i):
        for side, cols in enumerate((lo, hi)):
            for t in range(n_tiles // 2):
                rs_first(i, side * (n_tiles // 2) + t).wait_recv()
            rs_add(i, opp, cols, ra[i, 0, :, cols])
            rs_ring(i, side).start()

    def rs_c(i):
        rs_d2d(i, 1).wait_recv()
        rs_add(i, right, every, ra[i, 1])
        rs_ring(i, 2).start()
        rs_d2d(i, 2).wait_recv()
        rs_add(i, left, every, ra[i, 2])
        rs_ring(i, 3).start()

    def rs_d(i):
        rs_ring(i, 0).wait_recv()
        rs_add(i, right, lo, rb[i, 0])
        rs_ring(i, 4).start()
        rs_ring(i, 1).wait_recv()
        rs_add(i, left, hi, rb[i, 1])
        rs_ring(i, 5).start()

    def rs_e(i):
        rs_d2d(i, 3).wait_recv()
        for kind in range(2, 6):
            rs_ring(i, kind).wait_recv()
        for role in range(1, 4):
            rs_d2d(i, role).wait_send()
        for t in range(n_tiles):
            rs_first(i, t).wait_send()
        for kind in range(6):
            rs_ring(i, kind).wait_send()
        return (part[i, rows(0, me), :] + ra[i, 3]) + (rc[i, 0] + rc[i, 1])

    bufs = (n2, n2, cc, cc, n1, n1, ee, ee)
    f_pos = (1, 1, 2, 2, 0, 0, 3, 3)
    f_out = (f_x1, f_x2, f_dy1, f_dy2)

    def ag_msg(i, kind, fin, receive=False):
        buf = fbuf.at[f_pos[i]] if fin else bufs[i]
        if receive:
            whos = (left, right, partner, opp, opp, lax.rem(partner + tp - 2, tp), lax.rem(partner + 2, tp),
                    lax.rem(partner + chips, tp), lax.rem(partner + chips, tp))
        else:
            whos = (me, me, me, left, right, left, right, opp, opp)
        cols = (every, every, every, lo, hi, every, every, lo, hi)[kind]
        dev = (right, left, partner, right, left, partner, partner, partner, partner)[kind]
        ref = buf.at[rows(i % 2, whos[kind]), cols]
        return rcopy(ref, ref, ag_send.at[i, kind], ag_recv.at[i, kind], dev)

    def ag_f(i, fin=False):
        for kind in range(3):
            ag_msg(i, kind, fin).start()

    def ag_g(i, fin=False):
        ag_msg(i, 0, fin, True).wait_recv()
        ag_msg(i, 3, fin).start()
        ag_msg(i, 5, fin).start()
        ag_msg(i, 1, fin, True).wait_recv()
        ag_msg(i, 4, fin).start()
        ag_msg(i, 6, fin).start()

    def ag_h(i, fin=False):
        ag_msg(i, 3, fin, True).wait_recv()
        ag_msg(i, 7, fin).start()
        ag_msg(i, 4, fin, True).wait_recv()
        ag_msg(i, 8, fin).start()

    def fin_copy(i):
        r = halves[i % 2]
        return pltpu.make_async_copy(fbuf.at[f_pos[i], r], f_out[f_pos[i]].at[r], fin_sem.at[i])

    def ag_i(i, fin=False):
        for kind in (2, 5, 6, 7, 8):
            ag_msg(i, kind, fin, True).wait_recv()
        for kind in range(9):
            ag_msg(i, kind, fin).wait_send()
        if fin:
            fin_copy(i).start()
        if fin and i < 4:
            @pl.loop(0, ht // chunk)
            def _(b):
                r = pl.ds(pl.multiple_of((i % 2) * ht + b * chunk, chunk), chunk)
                got = fbuf[f_pos[i], r, :]
                bufs[i][r, :] = (rms(got)[0] if i < 2 else got).astype(BF16)

    def fin_start(i, value):
        fbuf[f_pos[i], rows(i % 2, me), :] = value
        ag_f(i, True)

    def out_copy(k, hb, src, dst, layer):
        r = halves[hb]
        return pltpu.make_async_copy(src.at[r], dst.at[layer, r], out_sem.at[k, hb])

    def rms(x_val):
        inv = lax.rsqrt(jnp.mean(x_val * x_val, axis=-1, keepdims=True) + EPS)
        return x_val * inv, inv

    def rms_back(x_val, grad):
        norm, inv = rms(x_val)
        return inv * (grad - norm * jnp.mean(grad * norm, axis=-1, keepdims=True))

    barrier = pltpu.get_barrier_semaphore()
    for other in (partner, right, left):
        pl.semaphore_signal(barrier, inc=1, device_id={'tp': other}, device_id_type=MESH)
    y_loads = [pltpu.make_async_copy(y1_h.at[halves[hb]], part.at[4 + hb], in_sem.at[hb]) for hb in range(2)]
    d_loads = [pltpu.make_async_copy(dy2_h.at[halves[hb]], part.at[6 + hb], in_sem.at[2 + hb]) for hb in range(2)]
    loads = []
    for hb in range(2):
        r = rows(hb, me)
        for k, (src, dst) in enumerate(((y1_h, x1.at[1, hb]), (y2_h, x2.at[1, hb]), (dy1_h, dy1.at[hb]), (dy2_h, dy2.at[hb]))):
            loads.append(pltpu.make_async_copy(src.at[r], dst, in_sem.at[4 + 4 * hb + k]))
    first = w_copies(0)
    y_loads[0].start()
    first[0].start()
    y_loads[0].wait()
    for cp in (first[1], y_loads[1], *d_loads, *loads, *first[2:]):
        cp.start()

    def rounded(dst, i, fn):
        @pl.loop(0, ht // chunk)
        def _(b):
            src = pl.ds(pl.multiple_of(b * chunk, chunk), chunk)
            dst[pl.ds(pl.multiple_of((i % 2) * ht + b * chunk, chunk), chunk), :] = fn(part[i, src, :]).astype(BF16)
    rounded(n1, 4, lambda x: rms(x)[0])
    pl.semaphore_wait(barrier, 3)

    def product(i, lhs_ref, w_ref):
        for t in range(n_tiles):
            part[i, :, tiles[t]] = mm(lhs_ref[halves[i % 2], :], w_ref[:, tiles[t]], NN)
            rs_first(i, t).start()

    def finish(i, slot, fin):
        hb = i % 2
        mine = rows(hb, me)
        total = rs_e(i)
        if i < 2:
            new = x2[1 - slot, hb] - total
            x2[slot, hb] = new
        elif i < 4:
            new = dy1[hb] + rms_back(x1[1 - slot, hb], total)
            dy1[hb] = new
        elif i < 6:
            new = x1[1 - slot, hb] - total
            x1[slot, hb] = new
        else:
            new = dy2[hb] + rms_back(x2[slot, hb], total)
            dy2[hb] = new

        def send_b():
            bufs[i][mine, :] = (rms(new)[0] if i in (0, 1, 4, 5) else new).astype(BF16)
            ag_f(i)
        if fin is True:
            fin_start(i, new)
        elif fin is False:
            send_b()
        else:
            pl.when(fin)(lambda: fin_start(i, new))
            pl.when(jnp.logical_not(fin))(send_b)

    def either(fn, i, end):
        pl.when(end)(lambda: fn(i, True))
        pl.when(jnp.logical_not(end))(lambda: fn(i))

    @pl.loop(0, n_layers)
    def _(step):
        layer = n_layers - 1 - step
        slot = lax.rem(step, 2)
        w1_s, w2_s, wqkv_s, wo_s = w1.at[slot], w2.at[slot], wqkv.at[slot], wo.at[slot]
        later = step > 0
        more = step < n_layers - 1
        end = step == n_layers - 1
        now = w_copies(step)

        def compute(i):
            hb = i % 2
            r = halves[hb]
            if i == 0:
                now[0].wait()

                @pl.when(more)
                def _():
                    for cp in w_copies(step + 1):
                        cp.start()
            if i < 2:
                out_copy(0, hb, n1, n1_o, layer).start()
                pre = mm(n1[r, :], w1_s[...], NT)
                tan = jnp.tanh(GELU_C * (pre + GELU_A * (pre * pre * pre)))
                cdf = 0.5 * (1.0 + tan)
                h_s[r, :] = (pre * cdf).astype(BF16)
                gp[r, :] = cdf + pre * (0.5 * GELU_C) * (1.0 - tan * tan) * (1.0 + (3.0 * GELU_A) * (pre * pre))
                out_copy(1, hb, h_s, h_o, layer).start()
            elif i < 4:
                out_copy(2, hb, ee, e_o, layer).start()
                u_s[r, :] = (gp[r, :] * mm(ee[r, :], w2_s[...], NT)).astype(BF16)
                out_copy(3, hb, u_s, u_o, layer).start()
            elif i < 6:
                if i == 4:
                    for cp in now[2:]:
                        cp.wait()
                out_copy(4, hb, n2, n2_o, layer).start()
                qkv[r, :] = mm(n2[r, :], wqkv_s[...], NT).astype(BF16)
                key, val = qkv[r, qw:qw + hd], qkv[r, qw + hd:qw + 2 * hd]
                seen = mask[hb] > 0.5
                for head in range(heads):
                    cols = pl.ds(head * hd, hd)
                    sc = jnp.where(seen, mm(qkv[r, cols], key, NT) * scale, MASK_VALUE)
                    ex = jnp.exp(sc - jnp.max(sc, axis=-1, keepdims=True))
                    pr = ex / jnp.sum(ex, axis=-1, keepdims=True)
                    probs[head, r, :] = pr
                    att[r, cols] = mm(pr.astype(BF16), val, NN).astype(BF16)
                out_copy(5, hb, att, a_o, layer).start()
            else:
                out_copy(6, hb, cc, c_o, layer).start()
                d_att = mm(cc[r, :], wo_s[...], NT).astype(BF16)
                key, val = qkv[r, qw:qw + hd], qkv[r, qw + hd:qw + 2 * hd]
                d_key = jnp.zeros((ht, hd), F32)
                d_val = jnp.zeros((ht, hd), F32)
                for head in range(heads):
                    cols = pl.ds(head * hd, hd)
                    da = d_att[:, head * hd:(head + 1) * hd]
                    pr = probs[head, r, :]
                    dp = mm(da, val, NT)
                    ds = (pr * (dp - jnp.sum(dp * pr, axis=-1, keepdims=True)) * scale).astype(BF16)
                    dqkv[r, cols] = mm(ds, key, NN).astype(BF16)
                    d_key = d_key + mm(ds, qkv[r, cols], TN)
                    d_val = d_val + mm(pr.astype(BF16), da, TN)
                dqkv[r, qw:qw + hd] = d_key.astype(BF16)
                dqkv[r, qw + hd:qw + 2 * hd] = d_val.astype(BF16)
                out_copy(7, hb, dqkv, d_o, layer).start()

        def send(i):
            hb = i % 2
            if i == 0:
                now[1].wait()
            product(i, (h_s, u_s, att, dqkv)[i // 2], (w2_s, w1_s, wo_s, wqkv_s)[i // 2])
            if 4 <= i < 6:
                out_copy(0, hb, n1, n1_o, layer).wait()
            if i >= 6:
                out_copy(2, hb, ee, e_o, layer).wait()
            rs_a(i)

        def guarded(fn, i, back):
            w = (i - back) % 8
            if i < back:
                pl.when(later)(lambda: fn(w))
            elif fn is rs_d:
                fn(w)
            else:
                either(fn, w, end)

        for i in range(8):
            if i < 2:
                pl.when(later)(lambda: finish((i - 2) % 8, 1 - slot, False))
            else:
                finish(i - 2, slot, end)
            compute(i)
            guarded(rs_d, i, 1)
            guarded(ag_h, i, 3)
            send(i)
            if i == 0:
                @pl.when(step == 0)
                def _():
                    y_loads[1].wait()
                    rounded(n1, 5, lambda x: rms(x)[0])
            rs_b(i)
            guarded(ag_g, i, 2)
            rs_c(i)
            guarded(ag_i, i, 3)
            if i == 1:
                @pl.when(step == 0)
                def _():
                    for hb in range(2):
                        d_loads[hb].wait()
                        rounded(ee, 6 + hb, lambda x: x)
                        row_id = lax.broadcasted_iota(jnp.int32, (ht, ht), 0)
                        col_id = lax.broadcasted_iota(jnp.int32, (ht, ht), 1)
                        seen = jnp.zeros((ht, ht), F32)
                        for b in range(ht // seq):
                            inside = ((row_id < (b + 1) * seq) & (col_id >= b * seq) & (col_id <= row_id)
                                      & (col_id < b * seq + lens[hb * (ht // seq) + b]))
                            seen = jnp.where(inside, 1.0, seen)
                        mask[hb] = seen
                    for cp in loads:
                        cp.wait()
        for hb in range(2):
            for k, src, dst in ((1, h_s, h_o), (3, u_s, u_o), (4, n2, n2_o), (5, att, a_o), (6, cc, c_o), (7, dqkv, d_o)):
                out_copy(k, hb, src, dst, layer).wait()

    last = (n_layers - 1) % 2
    rs_d(7)
    finish(6, last, True)
    ag_h(5, True)
    finish(7, last, True)
    ag_i(5, True)
    for i in (6, 7):
        ag_g(i, True)
    for i in (6, 7):
        ag_h(i, True)
    for i in (6, 7):
        ag_i(i, True)
    for i in range(8):
        fin_copy(i).wait()


def grad_kernel(parts, n1, n2, c_val, e_val, h_val, u_val, a_val, d_val, *refs):
    qw, hd = parts
    ends_in, (g_up, g_down, g_q, g_k, g_v, g_out), ends_out = refs[:4], refs[4:10], refs[10:]
    for src, dst in zip(ends_in, ends_out):
        dst[...] = src[...]
    g_up[0] = mm(u_val[0], n1[0], TN)
    g_down[0] = mm(h_val[0], e_val[0], TN)
    g_out[0] = mm(a_val[0], c_val[0], TN)
    g_all = mm(d_val[0], n2[0], TN)
    g_q[0] = g_all[:qw]
    g_k[0] = g_all[qw:qw + hd]
    g_v[0] = g_all[qw + hd:]


def solution(mesh):
    tp = mesh.shape['tp']
    assert tp == 8
    act_spec = P('dp', None, None)
    w_specs = (P(None, None, 'tp', None), P(None, None, 'tp', None), P(None, None, 'tp', None),
               P(None, 'tp', None, None), P(None, None, 'tp'), P(None, 'tp', None))
    g_specs = (P('dp', None, 'tp', None), P('dp', None, 'tp', None), P('dp', None, 'tp', None),
               P('dp', 'tp', None, None), P('dp', None, 'tp'), P('dp', 'tp', None))

    def local_fn(y_one, y_two, dy_one, dy_two, seq_lens, w_query, w_key, w_value, w_out, w_up, w_down):
        batch, seq, width = y_one.shape
        n_layers, _, heads, hd = w_query.shape
        assert batch == tp and w_key.shape[2] == 1
        tokens = batch * seq
        ff = w_down.shape[1]
        qw = heads * hd
        ht = tokens // 2
        own = ht // tp
        assert ht % seq == 0 and own % 16 == 0
        acts = [x.reshape(tokens, width) for x in (y_one, y_two, dy_one, dy_two)]

        def flip(w):
            return w.transpose(0, 2, 3, 1).reshape(n_layers, -1, width)
        weights = (w_up.transpose(0, 2, 1), w_down, flip(w_query), flip(w_key), flip(w_value), w_out.reshape(n_layers, qw, width))

        def stack(cols):
            return jax.ShapeDtypeStruct((n_layers, tokens, cols), BF16)
        any_spec = pl.BlockSpec(memory_space=pl.ANY)
        vm = pltpu.VMEM
        dma = pltpu.SemaphoreType.DMA
        scratch = [vm((tokens, width), BF16)] * 4 + [
            vm((2, ff, width), BF16), vm((2, ff, width), BF16), vm((2, qw + 2 * hd, width), BF16), vm((2, qw, width), BF16),
            vm((tokens, ff), BF16), vm((tokens, ff), BF16), vm((tokens, ff), F32),
            vm((tokens, qw + 2 * hd), BF16), vm((tokens, qw), BF16), vm((tokens, qw + 2 * hd), BF16),
            vm((heads, tokens, ht), F32), vm((2, ht, ht), F32),
            vm((2, 2, own, width), F32), vm((2, 2, own, width), F32), vm((2, own, width), F32), vm((2, own, width), F32),
            vm((8, ht, width), F32), vm((8, 4, own, width), F32), vm((8, 2, own, width // 2), F32), vm((8, 2, own, width), F32),
            vm((4, tokens, width), F32),
            dma((2, 6)), dma((12,)), dma((8, 2)), dma((8,)), dma((8, 14)), dma((8, 14)), dma((8, 9)), dma((8, 9))]
        *ends, n1, n2, c_val, e_val, h_val, u_val, a_val, d_val = pl.pallas_call(
            functools.partial(chain_kernel, (n_layers, tp, seq, width, heads, hd)),
            out_shape=(jax.ShapeDtypeStruct((tokens, width), F32),) * 4 + (stack(width), stack(width), stack(width), stack(width),
                       stack(ff), stack(ff), stack(qw), stack(qw + 2 * hd)),
            in_specs=[pl.BlockSpec(memory_space=pltpu.SMEM)] + [any_spec] * 10,
            out_specs=(any_spec,) * 12,
            scratch_shapes=scratch,
            compiler_params=pltpu.CompilerParams(collective_id=0, has_side_effects=True, vmem_limit_bytes=66_000_000),
            name='chain',
        )(seq_lens, *acts, *weights)

        col_tile = 512

        def wide():
            return pl.BlockSpec((1, tokens, col_tile), lambda layer, j: (layer, 0, j))

        def small(cols):
            return pl.BlockSpec((1, tokens, cols), lambda layer, j: (layer, 0, 0))
        g_rows = (ff, ff, qw, hd, hd, qw)
        moved = 2 * n_layers * tokens * (4 * width + 2 * ff + 2 * qw + 2 * hd) + 4 * n_layers * width * sum(g_rows)
        steps = n_layers * (width // col_tile)
        end_spec = pl.BlockSpec((tokens // steps, width), lambda layer, j: (layer * (width // col_tile) + j, 0))
        g_up, g_down, g_q, g_k, g_v, g_out, *ends = pl.pallas_call(
            functools.partial(grad_kernel, (qw, hd)),
            grid=(n_layers, width // col_tile),
            out_shape=tuple(jax.ShapeDtypeStruct((n_layers, r, width), F32) for r in g_rows) + (jax.ShapeDtypeStruct((tokens, width), F32),) * 4,
            in_specs=[wide()] * 4 + [small(ff), small(ff), small(qw), small(qw + 2 * hd)] + [end_spec] * 4,
            out_specs=tuple(pl.BlockSpec((1, r, col_tile), lambda layer, j: (layer, 0, j)) for r in g_rows) + (end_spec,) * 4,
            compiler_params=pltpu.CompilerParams(vmem_limit_bytes=60_000_000),
            cost_estimate=pl.CostEstimate(flops=2 * n_layers * tokens * width * sum(g_rows), bytes_accessed=moved, transcendentals=0),
            name='grads',
        )(n1, n2, c_val, e_val, h_val, u_val, a_val, d_val, *ends)

        def flip_back(g, like):
            return g.reshape(n_layers, -1, hd, width).transpose(0, 3, 1, 2).reshape(like.shape)
        dw_up, dw_down, dw_out = g_up.transpose(0, 2, 1), g_down, g_out.reshape(w_out.shape)
        dw_query, dw_key, dw_value = flip_back(g_q, w_query), flip_back(g_k, w_key), flip_back(g_v, w_value)
        ends = tuple(v.reshape(batch, seq, width) for v in ends)
        return ends + (dw_query, dw_key, dw_value, dw_out, dw_up, dw_down)

    return jax.shard_map(local_fn, mesh=mesh,
                         in_specs=(act_spec,) * 4 + (P('dp'),) + w_specs,
                         out_specs=(act_spec,) * 4 + g_specs,
                         check_vma=False)
```

```python
import functools

import jax
import jax.numpy as jnp
from jax import lax
from jax.experimental import pallas as pl
from jax.experimental.pallas import tpu as pltpu
from jax.sharding import PartitionSpec as P

F32 = jnp.float32
BF16 = jnp.bfloat16
EPS = 1e-5
ORDER = 'AEDPSHBGCI'
MASK_VALUE = -1e30
GELU_C = 0.7978845608028654
GELU_A = 0.044715
MESH = pl.DeviceIdType.MESH
NT = (((1,), (1,)), ((), ()))
NN = (((1,), (0,)), ((), ()))
TN = (((0,), (0,)), ((), ()))


def mm(lhs, rhs, dims):
    return lax.dot_general(lhs, rhs, dims, preferred_element_type=F32)


def chain_kernel(cfg, lens, y1_h, y2_h, dy1_h, dy2_h, w1_h, w2_h, wq_h, wk_h, wv_h, wo_h,
                 f_x1, f_x2, f_dy1, f_dy2, n1_o, n2_o, c_o, e_o, h_o, u_o, a_o, d_o,
                 n1, n2, cc, ee, w1, w2, wqkv, wo, h_s, u_s, gp, qkv, att, dqkv, probs, mask,
                 x1, x2, dy1, dy2, part, ra, rb, rc, fbuf,
                 w_sem, in_sem, out_sem, fin_sem, rs_send, rs_recv, ag_send, ag_recv):
    n_layers, tp, seq, width, heads, hd = cfg
    chips = tp // 2
    tokens = tp * seq
    ht = tokens // 2
    own = ht // tp
    hw = width // 2
    chunk = 32
    scale = hd ** -0.5
    qw = heads * hd
    me = lax.axis_index('tp')
    chip = me // 2
    core = me - 2 * chip
    partner = me + 1 - 2 * core
    right = lax.rem(me + 2, tp)
    left = lax.rem(me + tp - 2, tp)
    opp = lax.rem(me + chips, tp)
    lo, hi, every = pl.ds(0, hw), pl.ds(hw, hw), pl.ds(0, width)
    halves = (pl.ds(0, ht), pl.ds(ht, ht))

    def rows(hb, who):
        return pl.ds(pl.multiple_of(hb * ht + who * own, own), own)

    def rcopy(src, dst, send, recv, dev):
        return pltpu.make_async_remote_copy(src_ref=src, dst_ref=dst, send_sem=send, recv_sem=recv,
                                            device_id={'tp': dev}, device_id_type=MESH)

    def w_copies(step):
        layer = n_layers - 1 - step
        slot = lax.rem(step, 2)
        kw = wk_h.shape[1]
        return (pltpu.make_async_copy(w1_h.at[layer], w1.at[slot], w_sem.at[slot, 0]),
                pltpu.make_async_copy(w2_h.at[layer], w2.at[slot], w_sem.at[slot, 1]),
                pltpu.make_async_copy(wq_h.at[layer], wqkv.at[slot, pl.ds(0, qw)], w_sem.at[slot, 2]),
                pltpu.make_async_copy(wk_h.at[layer], wqkv.at[slot, pl.ds(qw, kw)], w_sem.at[slot, 3]),
                pltpu.make_async_copy(wv_h.at[layer], wqkv.at[slot, pl.ds(qw + kw, kw)], w_sem.at[slot, 4]),
                pltpu.make_async_copy(wo_h.at[layer], wo.at[slot], w_sem.at[slot, 5]))

    owners = (opp, right, left, me)

    def rs_d2d(i, role):
        theirs = owners[role] + 1 - 2 * core
        return rcopy(part.at[i, rows(0, theirs)], ra.at[i, role], rs_send.at[i, role], rs_recv.at[i, role], partner)

    def rs_ring(i, kind):
        who, cols, dst, dev = ((opp, lo, rb.at[i, 0], right), (opp, hi, rb.at[i, 1], left),
                               (right, hi, rc.at[i, 0, :, hi], right), (left, lo, rc.at[i, 1, :, lo], left),
                               (right, lo, rc.at[i, 0, :, lo], right), (left, hi, rc.at[i, 1, :, hi], left))[kind]
        return rcopy(part.at[i, rows(0, who), cols], dst, rs_send.at[i, 4 + kind], rs_recv.at[i, 4 + kind], dev)

    def rs_add(i, who, cols, extra):
        r = rows(0, who)
        part[i, r, cols] = part[i, r, cols] + extra

    n_tiles = 4
    tiles = [pl.ds(t * (width // n_tiles), width // n_tiles) for t in range(n_tiles)]

    def rs_first(i, t):
        theirs = opp + 1 - 2 * core
        pos = 10 + t
        return rcopy(part.at[i, rows(0, theirs), tiles[t]], ra.at[i, 0, :, tiles[t]], rs_send.at[i, pos], rs_recv.at[i, pos], partner)

    def rs_a(i):
        for role in range(1, 4):
            rs_d2d(i, role).start()

    def rs_b(i):
        for side, cols in enumerate((lo, hi)):
            for t in range(n_tiles // 2):
                rs_first(i, side * (n_tiles // 2) + t).wait_recv()
            rs_add(i, opp, cols, ra[i, 0, :, cols])
            rs_ring(i, side).start()

    def rs_c(i):
        rs_d2d(i, 1).wait_recv()
        rs_add(i, right, every, ra[i, 1])
        rs_ring(i, 2).start()
        rs_d2d(i, 2).wait_recv()
        rs_add(i, left, every, ra[i, 2])
        rs_ring(i, 3).start()

    def rs_d(i):
        rs_ring(i, 0).wait_recv()
        rs_add(i, right, lo, rb[i, 0])
        rs_ring(i, 4).start()
        rs_ring(i, 1).wait_recv()
        rs_add(i, left, hi, rb[i, 1])
        rs_ring(i, 5).start()

    def rs_e(i):
        rs_d2d(i, 3).wait_recv()
        for kind in range(2, 6):
            rs_ring(i, kind).wait_recv()
        for role in range(1, 4):
            rs_d2d(i, role).wait_send()
        for t in range(n_tiles):
            rs_first(i, t).wait_send()
        for kind in range(6):
            rs_ring(i, kind).wait_send()
        return (part[i, rows(0, me), :] + ra[i, 3]) + (rc[i, 0] + rc[i, 1])

    bufs = (n2, n2, cc, cc, n1, n1, ee, ee)
    f_pos = (1, 1, 2, 2, 0, 0, 3, 3)
    f_out = (f_x1, f_x2, f_dy1, f_dy2)

    def ag_msg(i, kind, fin, receive=False):
        buf = fbuf.at[f_pos[i]] if fin else bufs[i]
        if receive:
            whos = (left, right, partner, opp, opp, lax.rem(partner + tp - 2, tp), lax.rem(partner + 2, tp),
                    lax.rem(partner + chips, tp), lax.rem(partner + chips, tp))
        else:
            whos = (me, me, me, left, right, left, right, opp, opp)
        cols = (every, every, every, lo, hi, every, every, lo, hi)[kind]
        dev = (right, left, partner, right, left, partner, partner, partner, partner)[kind]
        ref = buf.at[rows(i % 2, whos[kind]), cols]
        return rcopy(ref, ref, ag_send.at[i, kind], ag_recv.at[i, kind], dev)

    def ag_f(i, fin=False):
        for kind in range(3):
            ag_msg(i, kind, fin).start()

    def ag_g(i, fin=False):
        ag_msg(i, 0, fin, True).wait_recv()
        ag_msg(i, 3, fin).start()
        ag_msg(i, 5, fin).start()
        ag_msg(i, 1, fin, True).wait_recv()
        ag_msg(i, 4, fin).start()
        ag_msg(i, 6, fin).start()

    def ag_h(i, fin=False):
        ag_msg(i, 3, fin, True).wait_recv()
        ag_msg(i, 7, fin).start()
        ag_msg(i, 4, fin, True).wait_recv()
        ag_msg(i, 8, fin).start()

    def fin_copy(i):
        r = halves[i % 2]
        return pltpu.make_async_copy(fbuf.at[f_pos[i], r], f_out[f_pos[i]].at[r], fin_sem.at[i])

    def ag_i(i, fin=False):
        for kind in (2, 5, 6, 7, 8):
            ag_msg(i, kind, fin, True).wait_recv()
        for kind in range(9):
            ag_msg(i, kind, fin).wait_send()
        if fin:
            fin_copy(i).start()
        if fin and i < 4:
            @pl.loop(0, ht // chunk)
            def _(b):
                r = pl.ds(pl.multiple_of((i % 2) * ht + b * chunk, chunk), chunk)
                got = fbuf[f_pos[i], r, :]
                bufs[i][r, :] = (rms(got)[0] if i < 2 else got).astype(BF16)

    def fin_start(i, value):
        fbuf[f_pos[i], rows(i % 2, me), :] = value
        ag_f(i, True)

    def out_copy(k, hb, src, dst, layer):
        r = halves[hb]
        return pltpu.make_async_copy(src.at[r], dst.at[layer, r], out_sem.at[k, hb])

    def rms(x_val):
        inv = lax.rsqrt(jnp.mean(x_val * x_val, axis=-1, keepdims=True) + EPS)
        return x_val * inv, inv

    def rms_back(x_val, grad):
        norm, inv = rms(x_val)
        return inv * (grad - norm * jnp.mean(grad * norm, axis=-1, keepdims=True))

    barrier = pltpu.get_barrier_semaphore()
    for other in (partner, right, left):
        pl.semaphore_signal(barrier, inc=1, device_id={'tp': other}, device_id_type=MESH)
    y_loads = [pltpu.make_async_copy(y1_h.at[halves[hb]], part.at[4 + hb], in_sem.at[hb]) for hb in range(2)]
    d_loads = [pltpu.make_async_copy(dy2_h.at[halves[hb]], part.at[6 + hb], in_sem.at[2 + hb]) for hb in range(2)]
    loads = []
    for hb in range(2):
        r = rows(hb, me)
        for k, (src, dst) in enumerate(((y1_h, x1.at[1, hb]), (y2_h, x2.at[1, hb]), (dy1_h, dy1.at[hb]), (dy2_h, dy2.at[hb]))):
            loads.append(pltpu.make_async_copy(src.at[r], dst, in_sem.at[4 + 4 * hb + k]))
    first = w_copies(0)
    y_loads[0].start()
    first[0].start()
    y_loads[0].wait()
    for cp in (first[1], y_loads[1], *d_loads, *loads, *first[2:]):
        cp.start()

    def rounded(dst, i, fn):
        @pl.loop(0, ht // chunk)
        def _(b):
            src = pl.ds(pl.multiple_of(b * chunk, chunk), chunk)
            dst[pl.ds(pl.multiple_of((i % 2) * ht + b * chunk, chunk), chunk), :] = fn(part[i, src, :]).astype(BF16)
    rounded(n1, 4, lambda x: rms(x)[0])
    pl.semaphore_wait(barrier, 3)

    def product(i, lhs_ref, w_ref):
        for t in range(n_tiles):
            part[i, :, tiles[t]] = mm(lhs_ref[halves[i % 2], :], w_ref[:, tiles[t]], NN)
            rs_first(i, t).start()

    def finish(i, slot, fin):
        hb = i % 2
        mine = rows(hb, me)
        total = rs_e(i)
        if i < 2:
            new = x2[1 - slot, hb] - total
            x2[slot, hb] = new
        elif i < 4:
            new = dy1[hb] + rms_back(x1[1 - slot, hb], total)
            dy1[hb] = new
        elif i < 6:
            new = x1[1 - slot, hb] - total
            x1[slot, hb] = new
        else:
            new = dy2[hb] + rms_back(x2[slot, hb], total)
            dy2[hb] = new

        def send_b():
            bufs[i][mine, :] = (rms(new)[0] if i in (0, 1, 4, 5) else new).astype(BF16)
            ag_f(i)
        if fin is True:
            fin_start(i, new)
        elif fin is False:
            send_b()
        else:
            pl.when(fin)(lambda: fin_start(i, new))
            pl.when(jnp.logical_not(fin))(send_b)

    def either(fn, i, end):
        pl.when(end)(lambda: fn(i, True))
        pl.when(jnp.logical_not(end))(lambda: fn(i))

    @pl.loop(0, n_layers)
    def _(step):
        layer = n_layers - 1 - step
        slot = lax.rem(step, 2)
        w1_s, w2_s, wqkv_s, wo_s = w1.at[slot], w2.at[slot], wqkv.at[slot], wo.at[slot]
        later = step > 0
        more = step < n_layers - 1
        end = step == n_layers - 1
        now = w_copies(step)

        def compute(i):
            hb = i % 2
            r = halves[hb]
            if i == 0:
                now[0].wait()

                @pl.when(more)
                def _():
                    for cp in w_copies(step + 1):
                        cp.start()
            if i < 2:
                out_copy(0, hb, n1, n1_o, layer).start()
                pre = mm(n1[r, :], w1_s[...], NT)
                tan = jnp.tanh(GELU_C * (pre + GELU_A * (pre * pre * pre)))
                cdf = 0.5 * (1.0 + tan)
                h_s[r, :] = (pre * cdf).astype(BF16)
                gp[r, :] = cdf + pre * (0.5 * GELU_C) * (1.0 - tan * tan) * (1.0 + (3.0 * GELU_A) * (pre * pre))
                out_copy(1, hb, h_s, h_o, layer).start()
            elif i < 4:
                out_copy(2, hb, ee, e_o, layer).start()
                u_s[r, :] = (gp[r, :] * mm(ee[r, :], w2_s[...], NT)).astype(BF16)
                out_copy(3, hb, u_s, u_o, layer).start()
            elif i < 6:
                if i == 4:
                    for cp in now[2:]:
                        cp.wait()
                out_copy(4, hb, n2, n2_o, layer).start()
                qkv[r, :] = mm(n2[r, :], wqkv_s[...], NT).astype(BF16)
                key, val = qkv[r, qw:qw + hd], qkv[r, qw + hd:qw + 2 * hd]
                seen = mask[hb] > 0.5
                for head in range(heads):
                    cols = pl.ds(head * hd, hd)
                    sc = jnp.where(seen, mm(qkv[r, cols], key, NT) * scale, MASK_VALUE)
                    ex = jnp.exp(sc - jnp.max(sc, axis=-1, keepdims=True))
                    pr = ex / jnp.sum(ex, axis=-1, keepdims=True)
                    probs[head, r, :] = pr
                    att[r, cols] = mm(pr.astype(BF16), val, NN).astype(BF16)
                out_copy(5, hb, att, a_o, layer).start()
            else:
                out_copy(6, hb, cc, c_o, layer).start()
                d_att = mm(cc[r, :], wo_s[...], NT).astype(BF16)
                key, val = qkv[r, qw:qw + hd], qkv[r, qw + hd:qw + 2 * hd]
                d_key = jnp.zeros((ht, hd), F32)
                d_val = jnp.zeros((ht, hd), F32)
                for head in range(heads):
                    cols = pl.ds(head * hd, hd)
                    da = d_att[:, head * hd:(head + 1) * hd]
                    pr = probs[head, r, :]
                    dp = mm(da, val, NT)
                    ds = (pr * (dp - jnp.sum(dp * pr, axis=-1, keepdims=True)) * scale).astype(BF16)
                    dqkv[r, cols] = mm(ds, key, NN).astype(BF16)
                    d_key = d_key + mm(ds, qkv[r, cols], TN)
                    d_val = d_val + mm(pr.astype(BF16), da, TN)
                dqkv[r, qw:qw + hd] = d_key.astype(BF16)
                dqkv[r, qw + hd:qw + 2 * hd] = d_val.astype(BF16)
                out_copy(7, hb, dqkv, d_o, layer).start()

        def send(i):
            hb = i % 2
            if i == 0:
                now[1].wait()
            product(i, (h_s, u_s, att, dqkv)[i // 2], (w2_s, w1_s, wo_s, wqkv_s)[i // 2])
            if 4 <= i < 6:
                out_copy(0, hb, n1, n1_o, layer).wait()
            if i >= 6:
                out_copy(2, hb, ee, e_o, layer).wait()
            rs_a(i)

        def guarded(fn, i, back):
            w = (i - back) % 8
            if i < back:
                pl.when(later)(lambda: fn(w))
            elif fn is rs_d or fn is rs_c:
                fn(w)
            else:
                either(fn, w, end)

        def end_of(i, back):
            w = (i - back) % 8
            if i < back:
                pl.when(later)(lambda: finish(w, 1 - slot, False))
            else:
                finish(w, slot, end)

        def start_up(i):
            if i == 0:
                @pl.when(step == 0)
                def _():
                    y_loads[1].wait()
                    rounded(n1, 5, lambda x: rms(x)[0])

        ops = {'E': lambda i: end_of(i, 2), 'A': compute, 'D': lambda i: guarded(rs_d, i, 1), 'H': lambda i: guarded(ag_h, i, 3),
               'P': send, 'S': start_up, 'B': rs_b, 'G': lambda i: guarded(ag_g, i, 2), 'C': rs_c, 'c': lambda i: guarded(rs_c, i, 1),
               'I': lambda i: guarded(ag_i, i, 3), 'h': lambda i: guarded(ag_h, i, 2), 'e': lambda i: end_of(i, 1), 'i': lambda i: guarded(ag_i, i, 4)}
        for i in range(8):
            for op in ORDER:
                ops[op](i)
            if i == 1:
                @pl.when(step == 0)
                def _():
                    for hb in range(2):
                        d_loads[hb].wait()
                        rounded(ee, 6 + hb, lambda x: x)
                        row_id = lax.broadcasted_iota(jnp.int32, (ht, ht), 0)
                        col_id = lax.broadcasted_iota(jnp.int32, (ht, ht), 1)
                        seen = jnp.zeros((ht, ht), F32)
                        for b in range(ht // seq):
                            inside = ((row_id < (b + 1) * seq) & (col_id >= b * seq) & (col_id <= row_id)
                                      & (col_id < b * seq + lens[hb * (ht // seq) + b]))
                            seen = jnp.where(inside, 1.0, seen)
                        mask[hb] = seen
                    for cp in loads:
                        cp.wait()
        for hb in range(2):
            for k, src, dst in ((1, h_s, h_o), (3, u_s, u_o), (4, n2, n2_o), (5, att, a_o), (6, cc, c_o), (7, dqkv, d_o)):
                out_copy(k, hb, src, dst, layer).wait()

    last = (n_layers - 1) % 2
    if 'c' in ORDER:
        rs_c(7)
    rs_d(7)
    finish(6, last, True)
    ag_h(5, True)
    finish(7, last, True)
    ag_i(5, True)
    for i in (6, 7):
        ag_g(i, True)
    for i in (6, 7):
        ag_h(i, True)
    for i in (6, 7):
        ag_i(i, True)
    for i in range(8):
        fin_copy(i).wait()


def grad_kernel(parts, n1, n2, c_val, e_val, h_val, u_val, a_val, d_val, *refs):
    qw, hd = parts
    ends_in, (g_up, g_down, g_q, g_k, g_v, g_out), ends_out = refs[:4], refs[4:10], refs[10:]
    for src, dst in zip(ends_in, ends_out):
        dst[...] = src[...]
    g_up[0] = mm(u_val[0], n1[0], TN)
    g_down[0] = mm(h_val[0], e_val[0], TN)
    g_out[0] = mm(a_val[0], c_val[0], TN)
    g_all = mm(d_val[0], n2[0], TN)
    g_q[0] = g_all[:qw]
    g_k[0] = g_all[qw:qw + hd]
    g_v[0] = g_all[qw + hd:]


def solution(mesh):
    tp = mesh.shape['tp']
    assert tp == 8
    act_spec = P('dp', None, None)
    w_specs = (P(None, None, 'tp', None), P(None, None, 'tp', None), P(None, None, 'tp', None),
               P(None, 'tp', None, None), P(None, None, 'tp'), P(None, 'tp', None))
    g_specs = (P('dp', None, 'tp', None), P('dp', None, 'tp', None), P('dp', None, 'tp', None),
               P('dp', 'tp', None, None), P('dp', None, 'tp'), P('dp', 'tp', None))

    def local_fn(y_one, y_two, dy_one, dy_two, seq_lens, w_query, w_key, w_value, w_out, w_up, w_down):
        batch, seq, width = y_one.shape
        n_layers, _, heads, hd = w_query.shape
        assert batch == tp and w_key.shape[2] == 1
        tokens = batch * seq
        ff = w_down.shape[1]
        qw = heads * hd
        ht = tokens // 2
        own = ht // tp
        assert ht % seq == 0 and own % 16 == 0
        acts = [x.reshape(tokens, width) for x in (y_one, y_two, dy_one, dy_two)]

        def flip(w):
            return w.transpose(0, 2, 3, 1).reshape(n_layers, -1, width)
        weights = (w_up.transpose(0, 2, 1), w_down, flip(w_query), flip(w_key), flip(w_value), w_out.reshape(n_layers, qw, width))

        def stack(cols):
            return jax.ShapeDtypeStruct((n_layers, tokens, cols), BF16)
        any_spec = pl.BlockSpec(memory_space=pl.ANY)
        vm = pltpu.VMEM
        dma = pltpu.SemaphoreType.DMA
        scratch = [vm((tokens, width), BF16)] * 4 + [
            vm((2, ff, width), BF16), vm((2, ff, width), BF16), vm((2, qw + 2 * hd, width), BF16), vm((2, qw, width), BF16),
            vm((tokens, ff), BF16), vm((tokens, ff), BF16), vm((tokens, ff), F32),
            vm((tokens, qw + 2 * hd), BF16), vm((tokens, qw), BF16), vm((tokens, qw + 2 * hd), BF16),
            vm((heads, tokens, ht), F32), vm((2, ht, ht), F32),
            vm((2, 2, own, width), F32), vm((2, 2, own, width), F32), vm((2, own, width), F32), vm((2, own, width), F32),
            vm((8, ht, width), F32), vm((8, 4, own, width), F32), vm((8, 2, own, width // 2), F32), vm((8, 2, own, width), F32),
            vm((4, tokens, width), F32),
            dma((2, 6)), dma((12,)), dma((8, 2)), dma((8,)), dma((8, 14)), dma((8, 14)), dma((8, 9)), dma((8, 9))]
        *ends, n1, n2, c_val, e_val, h_val, u_val, a_val, d_val = pl.pallas_call(
            functools.partial(chain_kernel, (n_layers, tp, seq, width, heads, hd)),
            out_shape=(jax.ShapeDtypeStruct((tokens, width), F32),) * 4 + (stack(width), stack(width), stack(width), stack(width),
                       stack(ff), stack(ff), stack(qw), stack(qw + 2 * hd)),
            in_specs=[pl.BlockSpec(memory_space=pltpu.SMEM)] + [any_spec] * 10,
            out_specs=(any_spec,) * 12,
            scratch_shapes=scratch,
            compiler_params=pltpu.CompilerParams(collective_id=0, has_side_effects=True, vmem_limit_bytes=66_000_000),
            name='chain',
        )(seq_lens, *acts, *weights)

        col_tile = 512

        def wide():
            return pl.BlockSpec((1, tokens, col_tile), lambda layer, j: (layer, 0, j))

        def small(cols):
            return pl.BlockSpec((1, tokens, cols), lambda layer, j: (layer, 0, 0))
        g_rows = (ff, ff, qw, hd, hd, qw)
        moved = 2 * n_layers * tokens * (4 * width + 2 * ff + 2 * qw + 2 * hd) + 4 * n_layers * width * sum(g_rows)
        steps = n_layers * (width // col_tile)
        end_spec = pl.BlockSpec((tokens // steps, width), lambda layer, j: (layer * (width // col_tile) + j, 0))
        g_up, g_down, g_q, g_k, g_v, g_out, *ends = pl.pallas_call(
            functools.partial(grad_kernel, (qw, hd)),
            grid=(n_layers, width // col_tile),
            out_shape=tuple(jax.ShapeDtypeStruct((n_layers, r, width), F32) for r in g_rows) + (jax.ShapeDtypeStruct((tokens, width), F32),) * 4,
            in_specs=[wide()] * 4 + [small(ff), small(ff), small(qw), small(qw + 2 * hd)] + [end_spec] * 4,
            out_specs=tuple(pl.BlockSpec((1, r, col_tile), lambda layer, j: (layer, 0, j)) for r in g_rows) + (end_spec,) * 4,
            compiler_params=pltpu.CompilerParams(vmem_limit_bytes=60_000_000),
            cost_estimate=pl.CostEstimate(flops=2 * n_layers * tokens * width * sum(g_rows), bytes_accessed=moved, transcendentals=0),
            name='grads',
        )(n1, n2, c_val, e_val, h_val, u_val, a_val, d_val, *ends)

        def flip_back(g, like):
            return g.reshape(n_layers, -1, hd, width).transpose(0, 3, 1, 2).reshape(like.shape)
        dw_up, dw_down, dw_out = g_up.transpose(0, 2, 1), g_down, g_out.reshape(w_out.shape)
        dw_query, dw_key, dw_value = flip_back(g_q, w_query), flip_back(g_k, w_key), flip_back(g_v, w_value)
        ends = tuple(v.reshape(batch, seq, width) for v in ends)
        return ends + (dw_query, dw_key, dw_value, dw_out, dw_up, dw_down)

    return jax.shard_map(local_fn, mesh=mesh,
                         in_specs=(act_spec,) * 4 + (P('dp'),) + w_specs,
                         out_specs=(act_spec,) * 4 + g_specs,
                         check_vma=False)
```

```python
import functools

import jax
import jax.numpy as jnp
from jax import lax
from jax.experimental import pallas as pl
from jax.experimental.pallas import tpu as pltpu
from jax.sharding import PartitionSpec as P

F32 = jnp.float32
BF16 = jnp.bfloat16
EPS = 1e-5
ORDER = 'AEDPSHBGCI'
MASK_VALUE = -1e30
GELU_C = 0.7978845608028654
GELU_A = 0.044715
MESH = pl.DeviceIdType.MESH
NT = (((1,), (1,)), ((), ()))
NN = (((1,), (0,)), ((), ()))
TN = (((0,), (0,)), ((), ()))


def mm(lhs, rhs, dims):
    return lax.dot_general(lhs, rhs, dims, preferred_element_type=F32)


def chain_kernel(cfg, lens, y1_h, y2_h, dy1_h, dy2_h, w1_h, w2_h, wq_h, wk_h, wv_h, wo_h,
                 f_x1, f_x2, f_dy1, f_dy2, n1_o, n2_o, c_o, e_o, h_o, u_o, a_o, d_o,
                 n1, n2, cc, ee, w1, w2, wqkv, wo, h_s, u_s, gp, qkv, att, dqkv, probs, mask,
                 x1, x2, dy1, dy2, part, ra, rb, rc, fbuf,
                 w_sem, in_sem, out_sem, fin_sem, rs_send, rs_recv, ag_send, ag_recv):
    n_layers, tp, seq, width, heads, hd = cfg
    chips = tp // 2
    tokens = tp * seq
    ht = tokens // 2
    own = ht // tp
    hw = width // 2
    chunk = 32
    scale = hd ** -0.5
    qw = heads * hd
    me = lax.axis_index('tp')
    chip = me // 2
    core = me - 2 * chip
    partner = me + 1 - 2 * core
    right = lax.rem(me + 2, tp)
    left = lax.rem(me + tp - 2, tp)
    opp = lax.rem(me + chips, tp)
    lo, hi, every = pl.ds(0, hw), pl.ds(hw, hw), pl.ds(0, width)
    halves = (pl.ds(0, ht), pl.ds(ht, ht))

    def rows(hb, who):
        return pl.ds(pl.multiple_of(hb * ht + who * own, own), own)

    def rcopy(src, dst, send, recv, dev):
        return pltpu.make_async_remote_copy(src_ref=src, dst_ref=dst, send_sem=send, recv_sem=recv,
                                            device_id={'tp': dev}, device_id_type=MESH)

    def w_copies(step):
        layer = n_layers - 1 - step
        slot = lax.rem(step, 2)
        kw = wk_h.shape[1]
        return (pltpu.make_async_copy(w1_h.at[layer], w1.at[slot], w_sem.at[slot, 0]),
                pltpu.make_async_copy(w2_h.at[layer], w2.at[slot], w_sem.at[slot, 1]),
                pltpu.make_async_copy(wq_h.at[layer], wqkv.at[slot, pl.ds(0, qw)], w_sem.at[slot, 2]),
                pltpu.make_async_copy(wk_h.at[layer], wqkv.at[slot, pl.ds(qw, kw)], w_sem.at[slot, 3]),
                pltpu.make_async_copy(wv_h.at[layer], wqkv.at[slot, pl.ds(qw + kw, kw)], w_sem.at[slot, 4]),
                pltpu.make_async_copy(wo_h.at[layer], wo.at[slot], w_sem.at[slot, 5]))

    owners = (opp, right, left, me)

    def rs_d2d(i, role):
        theirs = owners[role] + 1 - 2 * core
        return rcopy(part.at[i, rows(0, theirs)], ra.at[i, role], rs_send.at[i, role], rs_recv.at[i, role], partner)

    def rs_ring(i, kind):
        who, cols, dst, dev = ((opp, lo, rb.at[i, 0], right), (opp, hi, rb.at[i, 1], left),
                               (right, hi, rc.at[i, 0, :, hi], right), (left, lo, rc.at[i, 1, :, lo], left),
                               (right, lo, rc.at[i, 0, :, lo], right), (left, hi, rc.at[i, 1, :, hi], left))[kind]
        return rcopy(part.at[i, rows(0, who), cols], dst, rs_send.at[i, 4 + kind], rs_recv.at[i, 4 + kind], dev)

    def rs_add(i, who, cols, extra):
        r = rows(0, who)
        part[i, r, cols] = part[i, r, cols] + extra

    n_tiles = 4
    tiles = [pl.ds(t * (width // n_tiles), width // n_tiles) for t in range(n_tiles)]

    def rs_first(i, t):
        theirs = opp + 1 - 2 * core
        pos = 10 + t
        return rcopy(part.at[i, rows(0, theirs), tiles[t]], ra.at[i, 0, :, tiles[t]], rs_send.at[i, pos], rs_recv.at[i, pos], partner)

    def rs_a(i):
        for role in range(1, 4):
            rs_d2d(i, role).start()

    def rs_b(i):
        for side, cols in enumerate((lo, hi)):
            for t in range(n_tiles // 2):
                rs_first(i, side * (n_tiles // 2) + t).wait_recv()
            rs_add(i, opp, cols, ra[i, 0, :, cols])
            rs_ring(i, side).start()

    def rs_c(i):
        rs_d2d(i, 1).wait_recv()
        rs_add(i, right, every, ra[i, 1])
        rs_ring(i, 2).start()
        rs_d2d(i, 2).wait_recv()
        rs_add(i, left, every, ra[i, 2])
        rs_ring(i, 3).start()

    def rs_d(i):
        rs_ring(i, 0).wait_recv()
        rs_add(i, right, lo, rb[i, 0])
        rs_ring(i, 4).start()
        rs_ring(i, 1).wait_recv()
        rs_add(i, left, hi, rb[i, 1])
        rs_ring(i, 5).start()

    def rs_e(i):
        rs_d2d(i, 3).wait_recv()
        for kind in range(2, 6):
            rs_ring(i, kind).wait_recv()
        for role in range(1, 4):
            rs_d2d(i, role).wait_send()
        for t in range(n_tiles):
            rs_first(i, t).wait_send()
        for kind in range(6):
            rs_ring(i, kind).wait_send()
        return (part[i, rows(0, me), :] + ra[i, 3]) + (rc[i, 0] + rc[i, 1])

    bufs = (n2, n2, cc, cc, n1, n1, ee, ee)
    f_pos = (1, 1, 2, 2, 0, 0, 3, 3)
    f_out = (f_x1, f_x2, f_dy1, f_dy2)

    def ag_msg(i, kind, fin, receive=False):
        buf = fbuf.at[f_pos[i]] if fin else bufs[i]
        if receive:
            whos = (left, right, partner, opp, opp, lax.rem(partner + tp - 2, tp), lax.rem(partner + 2, tp),
                    lax.rem(partner + chips, tp), lax.rem(partner + chips, tp))
        else:
            whos = (me, me, me, left, right, left, right, opp, opp)
        cols = (every, every, every, lo, hi, every, every, lo, hi)[kind]
        dev = (right, left, partner, right, left, partner, partner, partner, partner)[kind]
        ref = buf.at[rows(i % 2, whos[kind]), cols]
        return rcopy(ref, ref, ag_send.at[i, kind], ag_recv.at[i, kind], dev)

    def ag_f(i, fin=False):
        for kind in range(3):
            ag_msg(i, kind, fin).start()

    def ag_g(i, fin=False):
        ag_msg(i, 0, fin, True).wait_recv()
        ag_msg(i, 3, fin).start()
        ag_msg(i, 5, fin).start()
        ag_msg(i, 1, fin, True).wait_recv()
        ag_msg(i, 4, fin).start()
        ag_msg(i, 6, fin).start()

    def ag_h(i, fin=False):
        ag_msg(i, 3, fin, True).wait_recv()
        ag_msg(i, 7, fin).start()
        ag_msg(i, 4, fin, True).wait_recv()
        ag_msg(i, 8, fin).start()

    def fin_copy(i):
        r = halves[i % 2]
        return pltpu.make_async_copy(fbuf.at[f_pos[i], r], f_out[f_pos[i]].at[r], fin_sem.at[i])

    def ag_i(i, fin=False):
        for kind in (2, 5, 6, 7, 8):
            ag_msg(i, kind, fin, True).wait_recv()
        for kind in range(9):
            ag_msg(i, kind, fin).wait_send()
        if fin:
            fin_copy(i).start()
        if fin and i < 4:
            @pl.loop(0, ht // chunk)
            def _(b):
                r = pl.ds(pl.multiple_of((i % 2) * ht + b * chunk, chunk), chunk)
                got = fbuf[f_pos[i], r, :]
                bufs[i][r, :] = (rms(got)[0] if i < 2 else got).astype(BF16)

    def fin_start(i, value):
        fbuf[f_pos[i], rows(i % 2, me), :] = value
        ag_f(i, True)

    def out_copy(k, hb, src, dst, layer):
        r = halves[hb]
        return pltpu.make_async_copy(src.at[r], dst.at[layer, r], out_sem.at[k, hb])

    def rms(x_val):
        inv = lax.rsqrt(jnp.mean(x_val * x_val, axis=-1, keepdims=True) + EPS)
        return x_val * inv, inv

    def rms_back(x_val, grad):
        norm, inv = rms(x_val)
        return inv * (grad - norm * jnp.mean(grad * norm, axis=-1, keepdims=True))

    barrier = pltpu.get_barrier_semaphore()
    for other in (partner, right, left):
        pl.semaphore_signal(barrier, inc=1, device_id={'tp': other}, device_id_type=MESH)
    y_loads = [pltpu.make_async_copy(y1_h.at[halves[hb]], part.at[4 + hb], in_sem.at[hb]) for hb in range(2)]
    d_loads = [pltpu.make_async_copy(dy2_h.at[halves[hb]], part.at[6 + hb], in_sem.at[2 + hb]) for hb in range(2)]
    loads = []
    for hb in range(2):
        r = rows(hb, me)
        for k, (src, dst) in enumerate(((y1_h, x1.at[1, hb]), (y2_h, x2.at[1, hb]), (dy1_h, dy1.at[hb]), (dy2_h, dy2.at[hb]))):
            loads.append(pltpu.make_async_copy(src.at[r], dst, in_sem.at[4 + 4 * hb + k]))
    first = w_copies(0)
    y_loads[0].start()
    first[0].start()
    y_loads[0].wait()
    for cp in (first[1], y_loads[1], *d_loads, *loads, *first[2:]):
        cp.start()

    def rounded(dst, i, fn):
        @pl.loop(0, ht // chunk)
        def _(b):
            src = pl.ds(pl.multiple_of(b * chunk, chunk), chunk)
            dst[pl.ds(pl.multiple_of((i % 2) * ht + b * chunk, chunk), chunk), :] = fn(part[i, src, :]).astype(BF16)
    rounded(n1, 4, lambda x: rms(x)[0])
    pl.semaphore_wait(barrier, 3)

    def product(i, lhs_ref, w_ref):
        for t in range(n_tiles):
            part[i, :, tiles[t]] = mm(lhs_ref[halves[i % 2], :], w_ref[:, tiles[t]], NN)
            rs_first(i, t).start()

    def finish(i, slot, fin):
        hb = i % 2
        mine = rows(hb, me)
        total = rs_e(i)
        if i < 2:
            new = x2[1 - slot, hb] - total
            x2[slot, hb] = new
        elif i < 4:
            new = dy1[hb] + rms_back(x1[1 - slot, hb], total)
            dy1[hb] = new
        elif i < 6:
            new = x1[1 - slot, hb] - total
            x1[slot, hb] = new
        else:
            new = dy2[hb] + rms_back(x2[slot, hb], total)
            dy2[hb] = new

        def send_b():
            bufs[i][mine, :] = (rms(new)[0] if i in (0, 1, 4, 5) else new).astype(BF16)
            ag_f(i)
        if fin is True:
            fin_start(i, new)
        elif fin is False:
            send_b()
        else:
            pl.when(fin)(lambda: fin_start(i, new))
            pl.when(jnp.logical_not(fin))(send_b)

    def either(fn, i, end):
        pl.when(end)(lambda: fn(i, True))
        pl.when(jnp.logical_not(end))(lambda: fn(i))

    @pl.loop(0, n_layers)
    def _(step):
        layer = n_layers - 1 - step
        slot = lax.rem(step, 2)
        w1_s, w2_s, wqkv_s, wo_s = w1.at[slot], w2.at[slot], wqkv.at[slot], wo.at[slot]
        later = step > 0
        more = step < n_layers - 1
        end = step == n_layers - 1
        now = w_copies(step)

        def compute(i):
            hb = i % 2
            r = halves[hb]
            if i == 0:
                now[0].wait()

                @pl.when(more)
                def _():
                    for cp in w_copies(step + 1):
                        cp.start()
            if i < 2:
                out_copy(0, hb, n1, n1_o, layer).start()
                pre = mm(n1[r, :], w1_s[...], NT)
                tan = jnp.tanh(GELU_C * (pre + GELU_A * (pre * pre * pre)))
                cdf = 0.5 * (1.0 + tan)
                h_s[r, :] = (pre * cdf).astype(BF16)
                gp[r, :] = cdf + pre * (0.5 * GELU_C) * (1.0 - tan * tan) * (1.0 + (3.0 * GELU_A) * (pre * pre))
                out_copy(1, hb, h_s, h_o, layer).start()
            elif i < 4:
                out_copy(2, hb, ee, e_o, layer).start()
                u_s[r, :] = (gp[r, :] * mm(ee[r, :], w2_s[...], NT)).astype(BF16)
                out_copy(3, hb, u_s, u_o, layer).start()
            elif i < 6:
                if i == 4:
                    for cp in now[2:]:
                        cp.wait()
                out_copy(4, hb, n2, n2_o, layer).start()
                qkv[r, :] = mm(n2[r, :], wqkv_s[...], NT).astype(BF16)
                key, val = qkv[r, qw:qw + hd], qkv[r, qw + hd:qw + 2 * hd]
                seen = mask[hb] > 0.5
                for head in range(heads):
                    cols = pl.ds(head * hd, hd)
                    sc = jnp.where(seen, mm(qkv[r, cols], key, NT) * scale, MASK_VALUE)
                    ex = jnp.exp(sc - jnp.max(sc, axis=-1, keepdims=True))
                    pr = ex / jnp.sum(ex, axis=-1, keepdims=True)
                    probs[head, r, :] = pr
                    att[r, cols] = mm(pr.astype(BF16), val, NN).astype(BF16)
                out_copy(5, hb, att, a_o, layer).start()
            else:
                out_copy(6, hb, cc, c_o, layer).start()
                d_att = mm(cc[r, :], wo_s[...], NT).astype(BF16)
                key, val = qkv[r, qw:qw + hd], qkv[r, qw + hd:qw + 2 * hd]
                d_key = jnp.zeros((ht, hd), F32)
                d_val = jnp.zeros((ht, hd), F32)
                for head in range(heads):
                    cols = pl.ds(head * hd, hd)
                    da = d_att[:, head * hd:(head + 1) * hd]
                    pr = probs[head, r, :]
                    dp = mm(da, val, NT)
                    ds = (pr * (dp - jnp.sum(dp * pr, axis=-1, keepdims=True)) * scale).astype(BF16)
                    dqkv[r, cols] = mm(ds, key, NN).astype(BF16)
                    d_key = d_key + mm(ds, qkv[r, cols], TN)
                    d_val = d_val + mm(pr.astype(BF16), da, TN)
                dqkv[r, qw:qw + hd] = d_key.astype(BF16)
                dqkv[r, qw + hd:qw + 2 * hd] = d_val.astype(BF16)
                out_copy(7, hb, dqkv, d_o, layer).start()

        def send(i):
            hb = i % 2
            if i == 0:
                now[1].wait()
            product(i, (h_s, u_s, att, dqkv)[i // 2], (w2_s, w1_s, wo_s, wqkv_s)[i // 2])
            if 4 <= i < 6:
                out_copy(0, hb, n1, n1_o, layer).wait()
            if i >= 6:
                out_copy(2, hb, ee, e_o, layer).wait()
            rs_a(i)

        def guarded(fn, i, back):
            w = (i - back) % 8
            if i < back:
                pl.when(later)(lambda: fn(w))
            elif fn is rs_d:
                fn(w)
            else:
                either(fn, w, end)

        def end_of(i, back):
            w = (i - back) % 8
            if i < back:
                pl.when(later)(lambda: finish(w, 1 - slot, False))
            else:
                finish(w, slot, end)

        def start_up(i):
            if i == 0:
                @pl.when(step == 0)
                def _():
                    y_loads[1].wait()
                    rounded(n1, 5, lambda x: rms(x)[0])

        ops = {'E': lambda i: end_of(i, 2), 'A': compute, 'D': lambda i: guarded(rs_d, i, 1), 'H': lambda i: guarded(ag_h, i, 3),
               'P': send, 'S': start_up, 'B': rs_b, 'G': lambda i: guarded(ag_g, i, 2), 'C': rs_c,
               'I': lambda i: guarded(ag_i, i, 3)}
        for i in range(8):
            for op in ORDER:
                ops[op](i)
            if i == 1:
                @pl.when(step == 0)
                def _():
                    for hb in range(2):
                        d_loads[hb].wait()
                        rounded(ee, 6 + hb, lambda x: x)
                        row_id = lax.broadcasted_iota(jnp.int32, (ht, ht), 0)
                        col_id = lax.broadcasted_iota(jnp.int32, (ht, ht), 1)
                        seen = jnp.zeros((ht, ht), F32)
                        for b in range(ht // seq):
                            inside = ((row_id < (b + 1) * seq) & (col_id >= b * seq) & (col_id <= row_id)
                                      & (col_id < b * seq + lens[hb * (ht // seq) + b]))
                            seen = jnp.where(inside, 1.0, seen)
                        mask[hb] = seen
                    for cp in loads:
                        cp.wait()
        for hb in range(2):
            for k, src, dst in ((1, h_s, h_o), (3, u_s, u_o), (4, n2, n2_o), (5, att, a_o), (6, cc, c_o), (7, dqkv, d_o)):
                out_copy(k, hb, src, dst, layer).wait()

    last = (n_layers - 1) % 2
    rs_d(7)
    finish(6, last, True)
    ag_h(5, True)
    finish(7, last, True)
    ag_i(5, True)
    for i in (6, 7):
        ag_g(i, True)
    for i in (6, 7):
        ag_h(i, True)
    for i in (6, 7):
        ag_i(i, True)
    for i in range(8):
        fin_copy(i).wait()


def grad_kernel(parts, n1, n2, c_val, e_val, h_val, u_val, a_val, d_val, *refs):
    qw, hd = parts
    ends_in, (g_up, g_down, g_q, g_k, g_v, g_out), ends_out = refs[:4], refs[4:10], refs[10:]
    for src, dst in zip(ends_in, ends_out):
        dst[...] = src[...]
    g_up[0] = mm(u_val[0], n1[0], TN)
    g_down[0] = mm(h_val[0], e_val[0], TN)
    g_out[0] = mm(a_val[0], c_val[0], TN)
    g_all = mm(d_val[0], n2[0], TN)
    g_q[0] = g_all[:qw]
    g_k[0] = g_all[qw:qw + hd]
    g_v[0] = g_all[qw + hd:]


def solution(mesh):
    tp = mesh.shape['tp']
    assert tp == 8
    act_spec = P('dp', None, None)
    w_specs = (P(None, None, 'tp', None), P(None, None, 'tp', None), P(None, None, 'tp', None),
               P(None, 'tp', None, None), P(None, None, 'tp'), P(None, 'tp', None))
    g_specs = (P('dp', None, 'tp', None), P('dp', None, 'tp', None), P('dp', None, 'tp', None),
               P('dp', 'tp', None, None), P('dp', None, 'tp'), P('dp', 'tp', None))

    def local_fn(y_one, y_two, dy_one, dy_two, seq_lens, w_query, w_key, w_value, w_out, w_up, w_down):
        batch, seq, width = y_one.shape
        n_layers, _, heads, hd = w_query.shape
        assert batch == tp and w_key.shape[2] == 1
        tokens = batch * seq
        ff = w_down.shape[1]
        qw = heads * hd
        ht = tokens // 2
        own = ht // tp
        assert ht % seq == 0 and own % 16 == 0
        acts = [x.reshape(tokens, width) for x in (y_one, y_two, dy_one, dy_two)]

        def flip(w):
            return w.transpose(0, 2, 3, 1).reshape(n_layers, -1, width)
        weights = (w_up.transpose(0, 2, 1), w_down, flip(w_query), flip(w_key), flip(w_value), w_out.reshape(n_layers, qw, width))

        def stack(cols):
            return jax.ShapeDtypeStruct((n_layers, tokens, cols), BF16)
        any_spec = pl.BlockSpec(memory_space=pl.ANY)
        vm = pltpu.VMEM
        dma = pltpu.SemaphoreType.DMA
        scratch = [vm((tokens, width), BF16)] * 4 + [
            vm((2, ff, width), BF16), vm((2, ff, width), BF16), vm((2, qw + 2 * hd, width), BF16), vm((2, qw, width), BF16),
            vm((tokens, ff), BF16), vm((tokens, ff), BF16), vm((tokens, ff), F32),
            vm((tokens, qw + 2 * hd), BF16), vm((tokens, qw), BF16), vm((tokens, qw + 2 * hd), BF16),
            vm((heads, tokens, ht), F32), vm((2, ht, ht), F32),
            vm((2, 2, own, width), F32), vm((2, 2, own, width), F32), vm((2, own, width), F32), vm((2, own, width), F32),
            vm((8, ht, width), F32), vm((8, 4, own, width), F32), vm((8, 2, own, width // 2), F32), vm((8, 2, own, width), F32),
            vm((4, tokens, width), F32),
            dma((2, 6)), dma((12,)), dma((8, 2)), dma((8,)), dma((8, 14)), dma((8, 14)), dma((8, 9)), dma((8, 9))]
        *ends, n1, n2, c_val, e_val, h_val, u_val, a_val, d_val = pl.pallas_call(
            functools.partial(chain_kernel, (n_layers, tp, seq, width, heads, hd)),
            out_shape=(jax.ShapeDtypeStruct((tokens, width), F32),) * 4 + (stack(width), stack(width), stack(width), stack(width),
                       stack(ff), stack(ff), stack(qw), stack(qw + 2 * hd)),
            in_specs=[pl.BlockSpec(memory_space=pltpu.SMEM)] + [any_spec] * 10,
            out_specs=(any_spec,) * 12,
            scratch_shapes=scratch,
            compiler_params=pltpu.CompilerParams(collective_id=0, has_side_effects=True, vmem_limit_bytes=66_000_000),
            name='chain',
        )(seq_lens, *acts, *weights)

        col_tile = 1024

        def wide():
            return pl.BlockSpec((1, tokens, col_tile), lambda layer, j: (layer, 0, j))

        def small(cols):
            return pl.BlockSpec((1, tokens, cols), lambda layer, j: (layer, 0, 0))
        g_rows = (ff, ff, qw, hd, hd, qw)
        moved = 2 * n_layers * tokens * (4 * width + 2 * ff + 2 * qw + 2 * hd) + 4 * n_layers * width * sum(g_rows)
        steps = n_layers * (width // col_tile)
        end_spec = pl.BlockSpec((tokens // steps, width), lambda layer, j: (layer * (width // col_tile) + j, 0))
        g_up, g_down, g_q, g_k, g_v, g_out, *ends = pl.pallas_call(
            functools.partial(grad_kernel, (qw, hd)),
            grid=(n_layers, width // col_tile),
            out_shape=tuple(jax.ShapeDtypeStruct((n_layers, r, width), F32) for r in g_rows) + (jax.ShapeDtypeStruct((tokens, width), F32),) * 4,
            in_specs=[wide()] * 4 + [small(ff), small(ff), small(qw), small(qw + 2 * hd)] + [end_spec] * 4,
            out_specs=tuple(pl.BlockSpec((1, r, col_tile), lambda layer, j: (layer, 0, j)) for r in g_rows) + (end_spec,) * 4,
            compiler_params=pltpu.CompilerParams(vmem_limit_bytes=60_000_000),
            cost_estimate=pl.CostEstimate(flops=2 * n_layers * tokens * width * sum(g_rows), bytes_accessed=moved, transcendentals=0),
            name='grads',
        )(n1, n2, c_val, e_val, h_val, u_val, a_val, d_val, *ends)

        def flip_back(g, like):
            return g.reshape(n_layers, -1, hd, width).transpose(0, 3, 1, 2).reshape(like.shape)
        dw_up, dw_down, dw_out = g_up.transpose(0, 2, 1), g_down, g_out.reshape(w_out.shape)
        dw_query, dw_key, dw_value = flip_back(g_q, w_query), flip_back(g_k, w_key), flip_back(g_v, w_value)
        ends = tuple(v.reshape(batch, seq, width) for v in ends)
        return ends + (dw_query, dw_key, dw_value, dw_out, dw_up, dw_down)

    return jax.shard_map(local_fn, mesh=mesh,
                         in_specs=(act_spec,) * 4 + (P('dp'),) + w_specs,
                         out_specs=(act_spec,) * 4 + g_specs,
                         check_vma=False)
```
